256 devices in a mesh: base: 32 (over x, z_lo, core), chan: 8 (over y, z_hi).
Axes of the slice: x: 4, y: 4, z: 8 (z_hi: 2, z_lo: 4; z = z_hi * 4 + z_lo), core: 2. Of those that a mesh axis runs over, the one named last changes fastest.
Arguments:
- image0: float32 [2048, 2048], P(('base', 'chan')), may hold values from -6 to 6
- interp: float32 [32, 8, 256, 8, 256], P('base', 'chan'), may hold values from -0.375 to 0.375
- vis_weight: float32 [32, 8, 256, 8], P('base', 'chan'), may hold values from 0.2 to 5
- counts: int32 [32, 8, 256], P('base', 'chan'), may hold values from 1 to 8
- tile_index: int32 [32, 8, 256], P('base', 'chan'), may hold values from 0 to 63
Outputs:
- image_out: float32 [2048, 2048], P(('base', 'chan'))
- estimates: float32 [3], replicated
The draws below stay inside these ranges and needn't reach their ends.
Inputs may be any that keep to these rules, and one draw needn't show every extreme that they name: `tile_index`: slot s of a device belongs to the spectrum block of device s // 1 of base+chan, base index major; the entry numbers the tile within that block. `counts`: visibility v of a slot is live when v < count.
All inputs are finite; a program needn't handle non-finite values.
Results may differ from the reference program's by a relative error of at most 0.00023.
Values sent between devices are 32-bit elements; how exact they have to be, the bound alone decides.
No kernel may reach another device: no remote copies, remote signals or barrier semaphores. Data moves between devices by JAX's collectives and lax.ppermute only.
A program may use at most 64 MiB of HBM per device.

```python
import math
import jax
import jax.numpy as jnp
from jax import lax

N = 2048
TILE_V = 8
TILE_U = 32
VCAP = 8
TOUCH = 256
ITERS = 3
CAP = 1
TILES_OWN = 64
N_BASE = 32
N_CHAN = 8


def place_ends(values, stream_key, smallest, top_value):
    longest = values.shape.index(max(values.shape))
    spots = []
    for shift in (0, 1):
        where = [jax.random.randint(jax.random.fold_in(stream_key, axis), (), 0, length) for axis, length in enumerate(values.shape)]
        where[longest] = (where[longest] + shift) % values.shape[longest]
        spots.append(tuple(where))
    return values.at[spots[0]].set(smallest).at[spots[1]].set(top_value)


def shard_levels(stream_key, dims, shards, smallest, top_value):
    gain, own = 1.0, jax.random.fold_in(stream_key, 6)
    for dim, parts in shards:
        heights = jnp.exp(jax.random.uniform(jax.random.fold_in(own, dim), (parts,), jnp.float32, smallest / len(shards), top_value / len(shards)))
        gain = gain * jnp.repeat(heights, dims[dim] // parts).reshape([-1 if axis == dim else 1 for axis in range(len(dims))])
    return gain


def scatter_about(stream_key, extent, spread, most, cuts=(), kind=jnp.bfloat16):
    values = jax.random.normal(stream_key, extent, jnp.float32) * spread
    if len(cuts) > 0:
        values = shard_levels(stream_key, extent, cuts, -0.22, 0.18) * values
    return jnp.clip(values, min=-most, max=most).astype(kind)


def setup_inputs(seed: int = 0) -> dict:
    splits = jax.random.split(jax.random.key(seed), 6)
    image0 = scatter_about(splits[0], (N, N), 1.0, 6.0, ((0, 256),), jnp.float32)
    interp = scatter_about(splits[1], (N_BASE, N_CHAN, TOUCH, VCAP, TILE_V * TILE_U), (TILE_V * TILE_U) ** -0.5, 0.375, ((0, 32), (1, 8)), jnp.float32)
    vis_weight = jnp.clip(jnp.exp(math.log(5.0) - 3.218876 * jax.random.uniform(splits[2], (N_BASE, N_CHAN, TOUCH, VCAP), jnp.float32) ** shard_levels(splits[2], (N_BASE, N_CHAN, TOUCH, VCAP), ((0, 32), (1, 8)), -0.2, 0.2)), 0.2, 5.0)
    counts = place_ends(jax.random.randint(splits[3], (N_BASE, N_CHAN, TOUCH), 1, VCAP + 1), jax.random.fold_in(splits[3], 1), 1, VCAP).astype(jnp.int32)
    tile_index = place_ends(jax.random.randint(splits[4], (N_BASE, N_CHAN, TOUCH), 0, TILES_OWN), jax.random.fold_in(splits[4], 1), 0, TILES_OWN - 1).astype(jnp.int32)
    return {"image0": image0, "interp": interp, "vis_weight": vis_weight, "counts": counts, "tile_index": tile_index}


PRECISION_LEVEL = lax.Precision.HIGHEST

def spectrum_tiles(image):
    devices = N_BASE * N_CHAN
    spectrum = jnp.fft.fft2(image, norm='ortho')
    planes = []
    for plane in (jnp.real(spectrum), jnp.imag(spectrum)):
        held = plane.T.reshape(devices, N // devices // TILE_V, TILE_V, N // TILE_U, TILE_U)
        planes.append(held.transpose(0, 1, 3, 2, 4).reshape(devices * TILES_OWN, TILE_V * TILE_U))
    return jnp.stack(planes, axis=1)

def image_of(grid):
    devices = N_BASE * N_CHAN
    planes = []
    for member in range(2):
        held = grid[:, member, :].reshape(devices, N // devices // TILE_V, N // TILE_U, TILE_V, TILE_U)
        planes.append(held.transpose(0, 1, 3, 2, 4).reshape(N, N).T)
    spectrum = lax.complex(planes[0], planes[1])
    return jnp.real(jnp.fft.ifft2(spectrum, norm='ortho'))

def apply_normal(image, sample_weights, masked_weight, global_index):
    tiles = spectrum_tiles(image)

    def accumulate(grid, pieces):
        slot_weight_table, slot_valid_mask, slot_index = pieces
        sample_values = tiles[slot_index]
        visible_samples = jnp.einsum('gnz,gez->gen', slot_weight_table, sample_values, precision=PRECISION_LEVEL) * slot_valid_mask[:, None, :]
        gridded_plane = jnp.einsum('hbi,hyb->hyi', slot_weight_table, visible_samples, precision=PRECISION_LEVEL)
        return (grid.at[slot_index].add(gridded_plane), None)
    grid, unused = lax.scan(accumulate, jnp.zeros_like(tiles), (sample_weights, masked_weight, global_index))
    return image_of(grid)

def reference(image0, interp, vis_weight, counts, tile_index):
    devices = N_BASE * N_CHAN
    sample_weights = interp.reshape(devices, TOUCH, VCAP, TILE_V * TILE_U)
    live = (jnp.arange(VCAP, dtype=jnp.int32)[None, None, :] < counts.reshape(devices, TOUCH, 1)).astype(jnp.float32)
    masked_weight = vis_weight.reshape(devices, TOUCH, VCAP) * live
    owner = (jnp.arange(TOUCH, dtype=jnp.int32) // CAP).astype(jnp.int32)
    global_index = (owner[None, :] * TILES_OWN + tile_index.reshape(devices, TOUCH)).astype(jnp.int32)
    current = image0 / jnp.sqrt(jnp.sum(image0 * image0))
    found = []
    for iteration in range(ITERS):
        image = apply_normal(current, sample_weights, masked_weight, global_index)
        norm_value = jnp.sqrt(jnp.sum(image * image))
        found.append(norm_value)
        current = image / norm_value
    return (N * current, jnp.stack(found))
```

```python
import functools
import math

import jax
import jax.numpy as jnp
import ml_dtypes
import numpy as np
from jax import lax
from jax.experimental import pallas as pl
from jax.experimental.pallas import tpu as pltpu
from jax.sharding import PartitionSpec as P

AXES = ("base", "chan")
N = 2048
DEV = 256
ROWS = 8
CELLS = 256
SLOTS = 256
VCAP = 8
SAMPLES = SLOTS * VCAP
LANES = 128
MSG = 18
GROUP = 4
START_SCALE = 2.0**-11
NORM_LANE = 40
F32 = jnp.float32
BF16 = jnp.bfloat16
VMEM = pl.BlockSpec(memory_space=pltpu.VMEM)
ANY = pl.BlockSpec(memory_space=pl.ANY)


def chip_path():
    path = []
    for x in range(4):
        for step_y, y in enumerate(range(4) if x % 2 == 0 else range(3, -1, -1)):
            zs = range(8) if (x * 4 + step_y) % 2 == 0 else range(7, -1, -1)
            path.extend((x, y, z) for z in zs)
    return path


def block_places():
    places = [0] * DEV
    for o, (x, y, z) in enumerate(chip_path()):
        for core in range(2):
            place = (x * 8 + z % 4 * 2 + core) * 8 + y * 2 + z // 4
            places[o if core == 0 else DEV - 1 - o] = place
    return places


PLACES = block_places()
MIRROR = [(PLACES[o], PLACES[DEV - 1 - o]) for o in range(DEV)]
MIRROR_EDGE = [(PLACES[o], PLACES[(DEV - o) % DEV]) for o in range(DEV)]


def halves(table):
    high = table.astype(ml_dtypes.bfloat16)
    low = (table - high.astype(np.float64)).astype(ml_dtypes.bfloat16)
    return high, low


def turns(products, modulus):
    angle = 2.0 * np.pi * (np.asarray(products) % modulus) / modulus
    return np.cos(angle), np.sin(angle)


@functools.cache
def tables():
    out = {}
    index = np.arange(DEV)
    for name, rows in (("plain", index), ("placed", np.array(PLACES))):
        cos, sin = turns(rows[:, None] * index[None, :], DEV)
        out[name] = halves(np.concatenate([cos, sin], axis=1))
    small = np.arange(8)
    cos, sin = turns(small[:, None] * index[None, :], N)
    out["turn"] = np.concatenate([cos, sin], axis=0).astype(np.float32)
    cos8, sin8 = turns(small[:, None] * small[None, :], 8)
    eye = np.eye(8)
    cos, sin = np.kron(eye, cos8), np.kron(eye, sin8)
    out["eight_fwd"] = halves(np.block([[cos, sin], [-sin, cos]]))
    out["eight_inv"] = halves(np.block([[cos, -sin], [sin, cos]]))
    row = np.arange(64)
    tile = row % 8 * 8 + row // 8
    place = np.argsort(tile)
    flips = []
    for source in (63 - tile, (64 - tile) % 64):
        one = np.zeros((64, 64))
        one[row, place[source]] = 1.0
        flips.append(np.kron(np.diag([1.0, -1.0]), one))
    out["flip_tile"] = np.concatenate(flips, axis=0).astype(ml_dtypes.bfloat16)
    cell = np.arange(CELLS)
    target = (8 - cell // 32) % 8 * 32 + (32 - cell % 32) % 32
    flip = np.zeros((CELLS, CELLS))
    flip[target, cell] = 1.0
    out["flip_cell"] = flip.astype(ml_dtypes.bfloat16)
    spread = (index[:, None] % 32 == index[None, :] // 8).astype(ml_dtypes.bfloat16)
    out["spread"] = spread
    share = np.zeros((DEV, 8))
    share[: DEV // 2, :4] = 2.0
    share[DEV // 2 :, 1:5] = 2.0
    share[0, 0] = 1.0
    share[DEV // 2, 0] = 1.0
    share = np.repeat(share, ROWS, axis=1)
    out["share"] = np.concatenate([share, share], axis=1).astype(np.float32)
    return out


def split(x):
    high = x.astype(BF16)
    return high, (x - high.astype(F32)).astype(BF16)


def dot(a, b, dims=((1,), (0,))):
    return lax.dot_general(a, b, (dims, ((), ())), preferred_element_type=F32)


def dot3(a, b, dims=((1,), (0,))):
    (ah, al), (bh, bl) = a, b
    return dot(ah, bh, dims) + (dot(ah, bl, dims) + dot(al, bh, dims))


NT = ((1,), (1,))


def load_pair(high_ref, low_ref):
    return high_ref[...], low_ref[...]


def swap_chunks(x):
    chunk = lax.broadcasted_iota(jnp.int32, (8, LANES), 1) // 32
    blocks = {}
    for part in range(2):
        for a_high in range(2):
            for b_high in range(2):
                source = [
                    x[
                        part * 64 + (a_high * 4 + a) * 8 : part * 64 + (a_high * 4 + a) * 8 + 8,
                        b_high * LANES : (b_high + 1) * LANES,
                    ]
                    for a in range(4)
                ]
                for b in range(4):
                    made = None
                    for a in range(4):
                        shift = (a - b) * 32 % LANES
                        moved = source[a] if shift == 0 else pltpu.roll(source[a], shift, 1)
                        made = moved if made is None else jnp.where(chunk == a, moved, made)
                    blocks[part, b_high * 4 + b, a_high] = made
    rows = [
        jnp.concatenate([blocks[part, b, 0], blocks[part, b, 1]], axis=1)
        for part in range(2)
        for b in range(8)
    ]
    return jnp.concatenate(rows, axis=0)


def fold(x):
    squares = x * x
    total = None
    for i in range(x.shape[0] // 8):
        for j in range(x.shape[1] // LANES):
            piece = squares[i * 8 : i * 8 + 8, j * LANES : (j + 1) * LANES]
            total = piece if total is None else total + piece
    return total


def apply_matrix(spectrum, ah_ref, al_ref, mask_ref):
    parts = split(spectrum)
    row = lax.broadcasted_iota(jnp.int32, (LANES, 256), 0)
    tile = (row % 8 * 8 + row // 8 % 8).astype(F32)
    total = None
    for m in range(SAMPLES // 256):
        a = (ah_ref[pl.ds(m * 256, 256), :], al_ref[pl.ds(m * 256, 256), :])
        seen = dot3(parts, a, NT)
        weight = mask_ref[m : m + 1, :]
        wanted = mask_ref[8 + m : 9 + m, :]
        kept = jnp.where(tile == wanted, seen * weight, 0.0)
        added = dot3(split(kept), a)
        total = added if total is None else total + added
    return total


def mirrored(own_ref, other_ref, edge_ref, flip_tile_ref, flip_cell_ref):
    lane = lax.broadcasted_iota(jnp.int32, (LANES, CELLS), 1)
    other = other_ref[...]
    edge = jnp.concatenate([edge_ref[...], other[:, LANES:]], axis=1)
    other = jnp.where(lane < 32, edge, other)
    high, low = split(other)
    flips = flip_tile_ref[...]
    turned = dot(flips, high) + dot(flips, low)
    turned = jnp.where(lane % 32 == 0, turned[LANES:], turned[:LANES])
    high, low = split(turned)
    flip = flip_cell_ref[...]
    return 0.5 * (own_ref[...] + (dot(high, flip) + dot(low, flip)))


def pack_kernel(image_ref, interp_ref, weight_ref, marks_ref, th_ref, tl_ref, turn_ref,
                out_ref, norm_ref, held, extra, sems):
    pieces = 4
    size = SLOTS // pieces
    copies = [
        pltpu.make_async_copy(
            interp_ref.at[pl.ds(i * size, size)], held.at[pl.ds(i * size, size)], sems.at[i]
        )
        for i in range(pieces)
    ]
    for copy in copies:
        copy.start()
    image = image_ref[...]
    x = [image[:, q * 256 : (q + 1) * 256] for q in range(8)]
    squares = None
    for q in range(8):
        both = x[q][:, :LANES] ** 2 + x[q][:, LANES:] ** 2
        squares = both if squares is None else squares + both
    norm_ref[...] = squares
    re, im = [None] * 8, [None] * 8
    for c in range(5):
        cos = [math.cos(2.0 * math.pi * (c * q % 8) / 8) for q in range(8)]
        sin = [math.sin(2.0 * math.pi * (c * q % 8) / 8) for q in range(8)]
        re[c] = sum(x[q] * cos[q] for q in range(1, 8)) + x[0]
        im[c] = jnp.zeros_like(x[0]) if c % 4 == 0 else -sum(x[q] * sin[q] for q in range(1, 8))
        if 0 < c < 4:
            re[8 - c] = re[c]
            im[8 - c] = -im[c]
    turned_re, turned_im = [], []
    for c in range(8):
        cos, sin = turn_ref[c : c + 1, :], turn_ref[8 + c : 9 + c, :]
        turned_re.append(re[c] * cos + im[c] * sin)
        turned_im.append(im[c] * cos - re[c] * sin)
    plain = jnp.concatenate(turned_re + turned_im, axis=0)
    crossed = jnp.concatenate(turned_im + [-v for v in turned_re], axis=0)
    data = split(jnp.concatenate([plain, crossed], axis=1))
    columns = dot3(load_pair(th_ref, tl_ref), data, NT)
    out_ref[pl.ds(16, DEV, stride=MSG), :] = columns
    marks = jnp.concatenate(
        [jnp.zeros((8, SLOTS), F32), marks_ref[...], jnp.zeros((LANES - 16, SLOTS), F32)], axis=0
    )
    extra[...] = marks.T
    extra[:, :VCAP] = weight_ref[...]
    out_ref[pl.ds(17, DEV, stride=MSG), :] = extra[...]

    def move(group, carry):
        base = pl.multiple_of(group * (GROUP * MSG), 8)
        for m in range(GROUP):
            for tile in range(2):
                out_ref[pl.ds(base + m * MSG + tile * 8, 8), :] = held[
                    group * GROUP + m, :, tile * LANES : (tile + 1) * LANES
                ]
        return carry

    groups = SLOTS // GROUP // pieces
    for i in range(pieces):
        copies[i].wait()
        lax.fori_loop(i * groups, (i + 1) * groups, move, 0, unroll=2)


def first_kernel(got_ref, th_ref, tl_ref, turn_ref, eh_ref, el_ref, spread_ref,
                 out_ref, ah_ref, al_ref, mask_ref):
    def unpack(group, carry):
        base = pl.multiple_of(group * (GROUP * MSG), 8)
        for pair in range(GROUP // 2):
            rows = []
            for m in (2 * pair, 2 * pair + 1):
                rows.append(
                    jnp.concatenate(
                        [got_ref[pl.ds(base + m * MSG + t * 8, 8), :] for t in range(2)], axis=1
                    )
                )
            high, low = split(jnp.concatenate(rows, axis=0))
            start = pl.multiple_of(group * 32 + pair * 16, 16)
            ah_ref[pl.ds(start, 16), :] = high
            al_ref[pl.ds(start, 16), :] = low
        return carry

    lax.fori_loop(0, SLOTS // GROUP, unpack, 0, unroll=2)

    marks = got_ref[pl.ds(17, DEV, stride=MSG), :].T[:16]
    chunk = lax.broadcasted_iota(jnp.int32, (16, SLOTS), 1) // 32
    stacked = jnp.concatenate([jnp.where(chunk == m, marks, 0.0) for m in range(8)], axis=0)
    high, low = split(stacked)
    lowest = (stacked - high.astype(F32) - low.astype(F32)).astype(BF16)
    spread = spread_ref[...]
    spread_marks = dot(high, spread) + (dot(low, spread) + dot(lowest, spread))
    sample = lax.broadcasted_iota(jnp.int32, (8, 256), 1) % 8
    row = lax.broadcasted_iota(jnp.int32, (8, 256), 0)
    for m in range(8):
        block = spread_marks[m * 16 : m * 16 + 16]
        weight = jnp.sum(jnp.where(sample == row, block[:8], 0.0), axis=0, keepdims=True)
        live = sample[:1].astype(F32) < block[9:10]
        mask_ref[m : m + 1, :] = jnp.where(live, weight, 0.0)
        mask_ref[8 + m : 9 + m, :] = block[8:9]

    columns = got_ref[pl.ds(16, DEV, stride=MSG), :].T
    both = dot3(split(columns), load_pair(th_ref, tl_ref))
    by_cos, by_sin = both[:, :DEV], both[:, DEV:]
    re = (by_cos[:64] + by_sin[64:]).reshape(8, 8, DEV)
    im = (by_cos[64:] - by_sin[:64]).reshape(8, 8, DEV)
    scale = START_SCALE / N
    cos, sin = turn_ref[:8, :] * scale, turn_ref[8:, :] * scale
    turned = jnp.concatenate([re * cos + im * sin, im * cos - re * sin], axis=0)
    spectrum = dot3(load_pair(eh_ref, el_ref), split(turned.reshape(LANES, DEV)))
    out_ref[...] = apply_matrix(swap_chunks(spectrum), ah_ref, al_ref, mask_ref)


def next_kernel(own_ref, other_ref, edge_ref, ah_ref, al_ref, mask_ref, ft_ref, fc_ref,
                out_ref, norm_ref):
    spectrum = mirrored(own_ref, other_ref, edge_ref, ft_ref, fc_ref)
    norm_ref[...] = fold(spectrum)
    out_ref[...] = apply_matrix(spectrum, ah_ref, al_ref, mask_ref)


def send_kernel(own_ref, other_ref, edge_ref, n0_ref, n1_ref, n2_ref, ft_ref, fc_ref,
                th_ref, tl_ref, turn_ref, eh_ref, el_ref, out_ref):
    spectrum = mirrored(own_ref, other_ref, edge_ref, ft_ref, fc_ref)
    norms = [jnp.sum(n) for n in (n0_ref[...], n1_ref[...], n2_ref[...], fold(spectrum))]
    data = dot3(load_pair(eh_ref, el_ref), split(swap_chunks(spectrum)))
    re = data[:64].reshape(8, 8, DEV)
    im = data[64:].reshape(8, 8, DEV)
    cos, sin = turn_ref[:8, :] * (1.0 / N), turn_ref[8:, :] * (1.0 / N)
    turned_re = (re * cos - im * sin).reshape(64, DEV)
    turned_im = (im * cos + re * sin).reshape(64, DEV)
    plain = jnp.concatenate([turned_re, turned_im], axis=0)
    crossed = jnp.concatenate([-turned_im, turned_re], axis=0)
    data = split(jnp.concatenate([plain, crossed], axis=1))
    out = dot3(load_pair(th_ref, tl_ref), data, NT)
    lane = lax.broadcasted_iota(jnp.int32, (DEV, LANES), 1)
    for i in range(4):
        out = jnp.where(lane == NORM_LANE + i, norms[i], out)
    out_ref[...] = out


def last_kernel(got_ref, share_ref, th_ref, tl_ref, turn_ref, image_ref, found_ref):
    got = got_ref[...]
    totals = jnp.sum(got, axis=0, keepdims=True)
    norms = [jnp.sqrt(totals[:, NORM_LANE + i : NORM_LANE + i + 1]) for i in range(4)]
    lane = lax.broadcasted_iota(jnp.int32, (1, LANES), 1)
    first = norms[1] / (norms[0] * START_SCALE)
    rest = [norms[2] / norms[1], norms[3] / norms[2]]
    found_ref[...] = jnp.where(lane == 0, first, jnp.where(lane == 1, rest[0], rest[1]))
    both = dot3(split((got * share_ref[...]).T), load_pair(th_ref, tl_ref))
    by_cos, by_sin = both[:, :DEV], both[:, DEV:]
    factor = float(N) / norms[3]
    re, im = [], []
    for c in range(5):
        here, there = slice(c * 8, c * 8 + 8), slice(64 + c * 8, 72 + c * 8)
        r = by_cos[here] - by_sin[there]
        i = by_cos[there] + by_sin[here]
        cos, sin = turn_ref[c : c + 1, :] * factor, turn_ref[8 + c : 9 + c, :] * factor
        re.append(r * cos - i * sin)
        im.append(i * cos + r * sin)
    for j in range(8):
        total = re[0]
        for c in range(1, 5):
            cos = math.cos(2.0 * math.pi * (c * j % 8) / 8)
            sin = math.sin(2.0 * math.pi * (c * j % 8) / 8)
            total = total + re[c] * cos - im[c] * sin
        image_ref[:, j * 256 : (j + 1) * 256] = total


def call(kernel, outs, in_specs, flops, moved, scratch=(), limit=24):
    return pl.pallas_call(
        kernel,
        out_shape=tuple(jax.ShapeDtypeStruct(s, t) for s, t in outs),
        in_specs=in_specs,
        out_specs=tuple(VMEM for _ in outs),
        scratch_shapes=list(scratch),
        compiler_params=pltpu.CompilerParams(vmem_limit_bytes=limit * 2**20),
        cost_estimate=pl.CostEstimate(flops=flops, bytes_accessed=moved, transcendentals=0),
    )


def exchange(message):
    rows = message.shape[0]
    out = lax.all_to_all(
        message.reshape(rows, 1, LANES), AXES, 0, 0, tiled=True, axis_index_groups=[PLACES]
    )
    return out.reshape(rows, LANES)


def mirror_exchange(grid):
    return (
        lax.ppermute(grid, AXES, MIRROR),
        lax.ppermute(grid[:, :LANES], AXES, MIRROR_EDGE),
    )


def per_device(image0, interp, vis_weight, counts, tile_index):
    t = {
        k: tuple(jnp.asarray(a) for a in v) if isinstance(v, tuple) else jnp.asarray(v)
        for k, v in tables().items()
    }
    marks = jnp.concatenate(
        [tile_index.reshape(1, SLOTS), counts.reshape(1, SLOTS), jnp.zeros((6, SLOTS), jnp.int32)]
    ).astype(F32)
    pack = call(
        pack_kernel,
        [((DEV * MSG, LANES), F32), ((8, LANES), F32)],
        [VMEM, ANY] + [VMEM] * 5,
        200_000_000,
        5_000_000,
        scratch=[
            pltpu.VMEM((SLOTS, VCAP, CELLS), F32),
            pltpu.VMEM((SLOTS, LANES), F32),
            pltpu.SemaphoreType.DMA((4,)),
        ],
    )
    message, n0 = pack(
        image0,
        interp.reshape(SLOTS, VCAP, CELLS),
        vis_weight.reshape(SLOTS, VCAP),
        marks,
        *t["plain"],
        t["turn"],
    )
    got = exchange(message)
    first = call(
        first_kernel,
        [
            ((LANES, CELLS), F32),
            ((SAMPLES, CELLS), BF16),
            ((SAMPLES, CELLS), BF16),
            ((16, 256), F32),
        ],
        [VMEM] * 7,
        1_000_000_000,
        5_000_000,
    )
    grid, a_high, a_low, mask = first(
        got, *t["placed"], t["turn"], *t["eight_fwd"], t["spread"]
    )
    norms = [n0]
    follow = call(
        next_kernel,
        [((LANES, CELLS), F32), ((8, LANES), F32)],
        [VMEM] * 8,
        1_000_000_000,
        3_000_000,
    )
    for _ in range(2):
        other, edge = mirror_exchange(grid)
        grid, norm = follow(
            grid, other, edge, a_high, a_low, mask, t["flip_tile"], t["flip_cell"]
        )
        norms.append(norm)
    other, edge = mirror_exchange(grid)
    send = call(send_kernel, [((DEV, LANES), F32)], [VMEM] * 13, 300_000_000, 1_500_000)
    (message,) = send(
        grid, other, edge, *norms, t["flip_tile"], t["flip_cell"],
        *t["placed"], t["turn"], *t["eight_inv"],
    )
    got = exchange(message)
    last = call(
        last_kernel,
        [((ROWS, N), F32), ((1, LANES), F32)],
        [VMEM] * 5,
        200_000_000,
        1_500_000,
    )
    image, found = last(got, t["share"], *t["plain"], t["turn"])
    return image, found[0, :3]


def solution(mesh):
    in_specs = (
        P(AXES, None),
        P("base", "chan", None, None, None),
        P("base", "chan", None, None),
        P("base", "chan", None),
        P("base", "chan", None),
    )
    return jax.shard_map(
        per_device, mesh=mesh, in_specs=in_specs, out_specs=(P(AXES, None), P()), check_vma=False
    )
```

```python
import functools
import math

import jax
import jax.numpy as jnp
import ml_dtypes
import numpy as np
from jax import lax
from jax.experimental import pallas as pl
from jax.experimental.pallas import tpu as pltpu
from jax.sharding import PartitionSpec as P

AXES = ("base", "chan")
N = 2048
DEV = 256
ROWS = 8
CELLS = 256
SLOTS = 256
VCAP = 8
SAMPLES = SLOTS * VCAP
LANES = 128
MSG = 18
GROUP = 4
START_SCALE = 2.0**-11
NORM_LANE = 40
PACK_LIMIT = 64_200_000
F32 = jnp.float32
BF16 = jnp.bfloat16
VMEM = pl.BlockSpec(memory_space=pltpu.VMEM)
HBM = pl.BlockSpec(memory_space=pltpu.HBM)


def chip_path():
    path = []
    for x in range(4):
        for step_y, y in enumerate(range(4) if x % 2 == 0 else range(3, -1, -1)):
            zs = range(8) if (x * 4 + step_y) % 2 == 0 else range(7, -1, -1)
            path.extend((x, y, z) for z in zs)
    return path


def block_places():
    places = [0] * DEV
    for o, (x, y, z) in enumerate(chip_path()):
        for core in range(2):
            place = (x * 8 + z % 4 * 2 + core) * 8 + y * 2 + z // 4
            places[o if core == 0 else DEV - 1 - o] = place
    return places


PLACES = block_places()
MIRROR = [(PLACES[o], PLACES[DEV - 1 - o]) for o in range(DEV)]
MIRROR_EDGE = [(PLACES[o], PLACES[(DEV - o) % DEV]) for o in range(DEV)]


def halves(table):
    high = table.astype(ml_dtypes.bfloat16)
    low = (table - high.astype(np.float64)).astype(ml_dtypes.bfloat16)
    return high, low


def turns(products, modulus):
    angle = 2.0 * np.pi * (np.asarray(products) % modulus) / modulus
    return np.cos(angle), np.sin(angle)


@functools.cache
def tables():
    out = {}
    index = np.arange(DEV)
    for name, rows in (("plain", index), ("placed", np.array(PLACES))):
        cos, sin = turns(rows[:, None] * index[None, :], DEV)
        out[name] = halves(np.concatenate([cos, sin], axis=1))
    small = np.arange(8)
    cos, sin = turns(small[:, None] * index[None, :], N)
    out["turn"] = np.concatenate([cos, sin], axis=0).astype(np.float32)
    cos8, sin8 = turns(small[:, None] * small[None, :], 8)
    eye = np.eye(8)
    cos, sin = np.kron(eye, cos8), np.kron(eye, sin8)
    out["eight_fwd"] = halves(np.block([[cos, sin], [-sin, cos]]))
    out["eight_inv"] = halves(np.block([[cos, -sin], [sin, cos]]))
    row = np.arange(64)
    tile = row % 8 * 8 + row // 8
    place = np.argsort(tile)
    flips = []
    for source in (63 - tile, (64 - tile) % 64):
        one = np.zeros((64, 64))
        one[row, place[source]] = 1.0
        flips.append(np.kron(np.diag([1.0, -1.0]), one))
    out["flip_tile"] = np.concatenate(flips, axis=0).astype(ml_dtypes.bfloat16)
    cell = np.arange(CELLS)
    target = (8 - cell // 32) % 8 * 32 + (32 - cell % 32) % 32
    flip = np.zeros((CELLS, CELLS))
    flip[target, cell] = 1.0
    out["flip_cell"] = flip.astype(ml_dtypes.bfloat16)
    spread = (index[:, None] % 32 == index[None, :] // 8).astype(ml_dtypes.bfloat16)
    out["spread"] = spread
    share = np.zeros((DEV, 8))
    share[: DEV // 2, :4] = 2.0
    share[DEV // 2 :, 1:5] = 2.0
    share[0, 0] = 1.0
    share[DEV // 2, 0] = 1.0
    share = np.repeat(share, ROWS, axis=1)
    out["share"] = np.concatenate([share, share], axis=1).astype(np.float32)
    return out


def split(x):
    high = x.astype(BF16)
    return high, (x - high.astype(F32)).astype(BF16)


def dot(a, b, dims=((1,), (0,))):
    return lax.dot_general(a, b, (dims, ((), ())), preferred_element_type=F32)


def dot3(a, b, dims=((1,), (0,))):
    (ah, al), (bh, bl) = a, b
    rows = ah.shape[0]
    both = dot(jnp.concatenate([ah, al], axis=0), bh, dims)
    return both[:rows] + (both[rows:] + dot(ah, bl, dims))


NT = ((1,), (1,))


def load_pair(high_ref, low_ref):
    return high_ref[...], low_ref[...]


def swap_chunks(x):
    chunk = lax.broadcasted_iota(jnp.int32, (8, LANES), 1) // 32
    blocks = {}
    for part in range(2):
        for a_high in range(2):
            for b_high in range(2):
                source = [
                    x[
                        part * 64 + (a_high * 4 + a) * 8 : part * 64 + (a_high * 4 + a) * 8 + 8,
                        b_high * LANES : (b_high + 1) * LANES,
                    ]
                    for a in range(4)
                ]
                for b in range(4):
                    made = None
                    for a in range(4):
                        shift = (a - b) * 32 % LANES
                        moved = source[a] if shift == 0 else pltpu.roll(source[a], shift, 1)
                        made = moved if made is None else jnp.where(chunk == a, moved, made)
                    blocks[part, b_high * 4 + b, a_high] = made
    rows = [
        jnp.concatenate([blocks[part, b, 0], blocks[part, b, 1]], axis=1)
        for part in range(2)
        for b in range(8)
    ]
    return jnp.concatenate(rows, axis=0)


def fold(x):
    squares = x * x
    total = None
    for i in range(x.shape[0] // 8):
        for j in range(x.shape[1] // LANES):
            piece = squares[i * 8 : i * 8 + 8, j * LANES : (j + 1) * LANES]
            total = piece if total is None else total + piece
    return total


def apply_matrix(spectrum, samples, mask_ref):
    parts = split(spectrum)
    row = lax.broadcasted_iota(jnp.int32, (LANES, 256), 0)
    tile = (row % 8 * 8 + row // 8 % 8).astype(F32)
    total = None
    for m in range(SAMPLES // 256):
        a = samples(m)
        seen = dot3(parts, a, NT)
        weight = mask_ref[m : m + 1, :]
        wanted = mask_ref[8 + m : 9 + m, :]
        kept = jnp.where(tile == wanted, seen * weight, 0.0)
        added = dot3(split(kept), a)
        total = added if total is None else total + added
    return total


def stored_samples(ah_ref, al_ref):
    return lambda m: (ah_ref[pl.ds(m * 256, 256), :], al_ref[pl.ds(m * 256, 256), :])


def pack_edge(grid):
    chunk = lax.broadcasted_iota(jnp.int32, (32, LANES), 1) // 32
    made = grid[:32, :LANES]
    for i in range(1, 4):
        moved = pltpu.roll(grid[i * 32 : i * 32 + 32, :LANES], i * 32, 1)
        made = jnp.where(chunk == i, moved, made)
    return made


def unpack_edge(edge):
    return jnp.concatenate(
        [edge] + [pltpu.roll(edge, LANES - i * 32, 1) for i in range(1, 4)], axis=0
    )


def mirrored(own_ref, other_ref, edge_ref, flip_tile_ref, flip_cell_ref):
    lane = lax.broadcasted_iota(jnp.int32, (LANES, CELLS), 1)
    other = other_ref[...]
    edge = jnp.concatenate([unpack_edge(edge_ref[...]), other[:, LANES:]], axis=1)
    other = jnp.where(lane < 32, edge, other)
    high, low = split(other)
    flips = flip_tile_ref[...]
    turned = dot(jnp.concatenate([flips, flips], axis=1), jnp.concatenate([high, low], axis=0))
    turned = jnp.where(lane % 32 == 0, turned[LANES:], turned[:LANES])
    high, low = split(turned)
    flip = flip_cell_ref[...]
    turned = dot(jnp.concatenate([high, low], axis=0), flip)
    return 0.5 * (own_ref[...] + (turned[:LANES] + turned[LANES:]))


def pack_kernel(image_hbm, interp_hbm, weight_hbm, index_hbm, counts_hbm, th_hbm, tl_hbm, turn_hbm,
                out_hbm, norm_ref, out_ref, image_ref, held, weight_ref, index_ref, counts_ref,
                th_ref, tl_ref, turn_ref, sems):
    pieces = 8
    size = SLOTS // pieces
    pairs = [
        (image_hbm, image_ref), (turn_hbm, turn_ref), (th_hbm, th_ref), (tl_hbm, tl_ref),
        (index_hbm, index_ref), (counts_hbm, counts_ref), (weight_hbm, weight_ref),
    ]
    pairs += [
        (interp_hbm.at[pl.ds(i * size, size)], held.at[pl.ds(i * size, size)])
        for i in range(pieces)
    ]
    copies = [
        pltpu.make_async_copy(source, target, sems.at[i])
        for i, (source, target) in enumerate(pairs)
    ]
    for copy in copies:
        copy.start()
    copies[0].wait()
    copies[1].wait()
    image = image_ref[...]
    x = [image[:, q * 256 : (q + 1) * 256] for q in range(8)]
    squares = None
    for q in range(8):
        both = x[q][:, :LANES] ** 2 + x[q][:, LANES:] ** 2
        squares = both if squares is None else squares + both
    norm_ref[...] = squares
    re, im = [None] * 8, [None] * 8
    for c in range(5):
        cos = [math.cos(2.0 * math.pi * (c * q % 8) / 8) for q in range(8)]
        sin = [math.sin(2.0 * math.pi * (c * q % 8) / 8) for q in range(8)]
        re[c] = sum(x[q] * cos[q] for q in range(1, 8)) + x[0]
        im[c] = jnp.zeros_like(x[0]) if c % 4 == 0 else -sum(x[q] * sin[q] for q in range(1, 8))
        if 0 < c < 4:
            re[8 - c] = re[c]
            im[8 - c] = -im[c]
    turned_re, turned_im = [], []
    for c in range(8):
        cos, sin = turn_ref[c : c + 1, :], turn_ref[8 + c : 9 + c, :]
        turned_re.append(re[c] * cos + im[c] * sin)
        turned_im.append(im[c] * cos - re[c] * sin)
    plain = jnp.concatenate(turned_re + turned_im, axis=0)
    crossed = jnp.concatenate(turned_im + [-v for v in turned_re], axis=0)
    data = split(jnp.concatenate([plain, crossed], axis=1))
    copies[2].wait()
    copies[3].wait()
    columns = dot3(load_pair(th_ref, tl_ref), data, NT)
    out_ref[pl.ds(16, DEV, stride=MSG), :] = columns
    for i in (4, 5, 6):
        copies[i].wait()
    marks = jnp.concatenate(
        [
            weight_ref[...],
            index_ref[...].astype(F32),
            counts_ref[...].astype(F32),
            jnp.zeros((LANES - 10, SLOTS), F32),
        ],
        axis=0,
    )
    out_ref[pl.ds(17, DEV, stride=MSG), :] = marks.T

    def move(group, carry):
        base = pl.multiple_of(group * (GROUP * MSG), 8)
        for m in range(GROUP):
            for tile in range(2):
                out_ref[pl.ds(base + m * MSG + tile * 8, 8), :] = held[
                    group * GROUP + m, :, tile * LANES : (tile + 1) * LANES
                ]
        return carry

    groups = SLOTS // GROUP // pieces
    rows = size * MSG
    sent = []
    for i in range(pieces):
        copies[7 + i].wait()
        lax.fori_loop(i * groups, (i + 1) * groups, move, 0, unroll=2)
        part = pl.ds(i * rows, rows)
        sent.append(
            pltpu.make_async_copy(out_ref.at[part], out_hbm.at[part], sems.at[15 + i])
        )
        sent[-1].start()
    for copy in sent:
        copy.wait()


def first_kernel(got_ref, th_ref, tl_ref, turn_ref, eh_ref, el_ref, spread_ref,
                 out_ref, edge_ref, ah_ref, al_ref, mask_ref):
    def samples(m):
        slots = [
            jnp.concatenate(
                [got_ref[pl.ds(slot * MSG + t * 8, 8), :] for t in range(2)], axis=1
            )
            for slot in range(m * 32, m * 32 + 32)
        ]
        high, low = split(jnp.concatenate(slots, axis=0))
        ah_ref[pl.ds(m * 256, 256), :] = high
        al_ref[pl.ds(m * 256, 256), :] = low
        return high, low

    marks = got_ref[pl.ds(17, DEV, stride=MSG), :].T[:16]
    chunk = lax.broadcasted_iota(jnp.int32, (16, SLOTS), 1) // 32
    stacked = jnp.concatenate([jnp.where(chunk == m, marks, 0.0) for m in range(8)], axis=0)
    high, low = split(stacked)
    lowest = (stacked - high.astype(F32) - low.astype(F32)).astype(BF16)
    spread = spread_ref[...]
    spread_marks = dot(high, spread) + (dot(low, spread) + dot(lowest, spread))
    sample = lax.broadcasted_iota(jnp.int32, (8, 256), 1) % 8
    row = lax.broadcasted_iota(jnp.int32, (8, 256), 0)
    for m in range(8):
        block = spread_marks[m * 16 : m * 16 + 16]
        weight = jnp.sum(jnp.where(sample == row, block[:8], 0.0), axis=0, keepdims=True)
        live = sample[:1].astype(F32) < block[9:10]
        mask_ref[m : m + 1, :] = jnp.where(live, weight, 0.0)
        mask_ref[8 + m : 9 + m, :] = block[8:9]

    columns = got_ref[pl.ds(16, DEV, stride=MSG), :].T
    both = dot3(split(columns), load_pair(th_ref, tl_ref))
    by_cos, by_sin = both[:, :DEV], both[:, DEV:]
    re = (by_cos[:64] + by_sin[64:]).reshape(8, 8, DEV)
    im = (by_cos[64:] - by_sin[:64]).reshape(8, 8, DEV)
    scale = START_SCALE / N
    cos, sin = turn_ref[:8, :] * scale, turn_ref[8:, :] * scale
    turned = jnp.concatenate([re * cos + im * sin, im * cos - re * sin], axis=0)
    spectrum = dot3(load_pair(eh_ref, el_ref), split(turned.reshape(LANES, DEV)))
    grid = apply_matrix(swap_chunks(spectrum), samples, mask_ref)
    out_ref[...] = grid
    edge_ref[...] = pack_edge(grid)


def next_kernel(own_ref, other_ref, edge_ref, ah_ref, al_ref, mask_ref, ft_ref, fc_ref,
                out_ref, edge_out_ref, norm_ref):
    spectrum = mirrored(own_ref, other_ref, edge_ref, ft_ref, fc_ref)
    norm_ref[...] = fold(spectrum)
    grid = apply_matrix(spectrum, stored_samples(ah_ref, al_ref), mask_ref)
    out_ref[...] = grid
    edge_out_ref[...] = pack_edge(grid)


def send_kernel(own_ref, other_ref, edge_ref, n0_ref, n1_ref, n2_ref, ft_ref, fc_ref,
                th_ref, tl_ref, turn_ref, eh_ref, el_ref, out_ref):
    spectrum = mirrored(own_ref, other_ref, edge_ref, ft_ref, fc_ref)
    norms = [jnp.sum(n) for n in (n0_ref[...], n1_ref[...], n2_ref[...], fold(spectrum))]
    data = dot3(load_pair(eh_ref, el_ref), split(swap_chunks(spectrum)))
    re = data[:64].reshape(8, 8, DEV)
    im = data[64:].reshape(8, 8, DEV)
    cos, sin = turn_ref[:8, :] * (1.0 / N), turn_ref[8:, :] * (1.0 / N)
    turned_re = (re * cos - im * sin).reshape(64, DEV)
    turned_im = (im * cos + re * sin).reshape(64, DEV)
    plain = jnp.concatenate([turned_re, turned_im], axis=0)
    crossed = jnp.concatenate([-turned_im, turned_re], axis=0)
    data = split(jnp.concatenate([plain, crossed], axis=1))
    out = dot3(load_pair(th_ref, tl_ref), data, NT)
    lane = lax.broadcasted_iota(jnp.int32, (DEV, LANES), 1)
    for i in range(4):
        out = jnp.where(lane == NORM_LANE + i, norms[i], out)
    out_ref[...] = out


def last_kernel(got_ref, share_ref, th_ref, tl_ref, turn_ref, image_ref, found_ref):
    got = got_ref[...]
    totals = jnp.sum(got, axis=0, keepdims=True)
    norms = [jnp.sqrt(totals[:, NORM_LANE + i : NORM_LANE + i + 1]) for i in range(4)]
    first = norms[1] / (norms[0] * START_SCALE)
    rest = [norms[2] / norms[1], norms[3] / norms[2]]
    lane = lax.broadcasted_iota(jnp.int32, (1, 3), 1)
    found_ref[...] = jnp.where(lane == 0, first, jnp.where(lane == 1, rest[0], rest[1]))
    both = dot3(split((got * share_ref[...]).T), load_pair(th_ref, tl_ref))
    by_cos, by_sin = both[:, :DEV], both[:, DEV:]
    factor = float(N) / norms[3]
    re, im = [], []
    for c in range(5):
        here, there = slice(c * 8, c * 8 + 8), slice(64 + c * 8, 72 + c * 8)
        r = by_cos[here] - by_sin[there]
        i = by_cos[there] + by_sin[here]
        cos, sin = turn_ref[c : c + 1, :] * factor, turn_ref[8 + c : 9 + c, :] * factor
        re.append(r * cos - i * sin)
        im.append(i * cos + r * sin)
    for j in range(8):
        total = re[0]
        for c in range(1, 5):
            cos = math.cos(2.0 * math.pi * (c * j % 8) / 8)
            sin = math.sin(2.0 * math.pi * (c * j % 8) / 8)
            total = total + re[c] * cos - im[c] * sin
        image_ref[:, j * 256 : (j + 1) * 256] = total


def call(kernel, outs, in_specs, flops, moved, scratch=(), limit=24 * 2**20, out_specs=None):
    return pl.pallas_call(
        kernel,
        out_shape=tuple(jax.ShapeDtypeStruct(s, t) for s, t in outs),
        in_specs=in_specs,
        out_specs=out_specs or tuple(VMEM for _ in outs),
        scratch_shapes=list(scratch),
        compiler_params=pltpu.CompilerParams(vmem_limit_bytes=limit),
        cost_estimate=pl.CostEstimate(flops=flops, bytes_accessed=moved, transcendentals=0),
    )


def exchange(message):
    rows = message.shape[0]
    out = lax.all_to_all(
        message.reshape(rows, 1, LANES), AXES, 0, 0, tiled=True, axis_index_groups=[PLACES]
    )
    return out.reshape(rows, LANES)


def mirror_exchange(grid, edge):
    edge = lax.ppermute(edge, AXES, MIRROR_EDGE)
    other = lax.ppermute(grid, AXES, MIRROR)
    return grid, other, edge


def per_device(image0, interp, vis_weight, counts, tile_index):
    t = {
        k: tuple(jnp.asarray(a) for a in v) if isinstance(v, tuple) else jnp.asarray(v)
        for k, v in tables().items()
    }
    pack = call(
        pack_kernel,
        [((DEV * MSG, LANES), F32), ((8, LANES), F32)],
        [HBM] * 8,
        200_000_000,
        5_000_000,
        scratch=[
            pltpu.VMEM((DEV * MSG, LANES), F32),
            pltpu.VMEM((ROWS, N), F32),
            pltpu.VMEM((SLOTS, VCAP, CELLS), F32),
            pltpu.VMEM((VCAP, SLOTS), F32),
            pltpu.VMEM((1, SLOTS), jnp.int32),
            pltpu.VMEM((1, SLOTS), jnp.int32),
            pltpu.VMEM((DEV, 2 * DEV), BF16),
            pltpu.VMEM((DEV, 2 * DEV), BF16),
            pltpu.VMEM((16, DEV), F32),
            pltpu.SemaphoreType.DMA((23,)),
        ],
        limit=PACK_LIMIT,
        out_specs=(HBM, VMEM),
    )
    message, n0 = pack(
        image0,
        interp.reshape(SLOTS, VCAP, CELLS),
        vis_weight.reshape(SLOTS, VCAP).T,
        tile_index.reshape(1, SLOTS),
        counts.reshape(1, SLOTS),
        *t["plain"],
        t["turn"],
    )
    got = exchange(message)
    first = call(
        first_kernel,
        [
            ((LANES, CELLS), F32),
            ((32, LANES), F32),
            ((SAMPLES, CELLS), BF16),
            ((SAMPLES, CELLS), BF16),
            ((16, 256), F32),
        ],
        [VMEM] * 7,
        1_000_000_000,
        5_000_000,
    )
    grid, edge, a_high, a_low, mask = first(
        got, *t["placed"], t["turn"], *t["eight_fwd"], t["spread"]
    )
    norms = [n0]
    follow = call(
        next_kernel,
        [((LANES, CELLS), F32), ((32, LANES), F32), ((8, LANES), F32)],
        [VMEM] * 8,
        1_000_000_000,
        3_000_000,
    )
    for _ in range(2):
        blocks = mirror_exchange(grid, edge)
        grid, edge, norm = follow(
            *blocks, a_high, a_low, mask, t["flip_tile"], t["flip_cell"]
        )
        norms.append(norm)
    blocks = mirror_exchange(grid, edge)
    send = call(send_kernel, [((DEV, LANES), F32)], [VMEM] * 13, 300_000_000, 1_500_000)
    (message,) = send(
        *blocks, *norms, t["flip_tile"], t["flip_cell"],
        *t["placed"], t["turn"], *t["eight_inv"],
    )
    got = exchange(message)
    last = call(
        last_kernel,
        [((ROWS, N), F32), ((1, 3), F32)],
        [VMEM] * 5,
        200_000_000,
        1_500_000,
    )
    image, found = last(got, t["share"], *t["plain"], t["turn"])
    return image, found.reshape(3)


def solution(mesh):
    in_specs = (
        P(AXES, None),
        P("base", "chan", None, None, None),
        P("base", "chan", None, None),
        P("base", "chan", None),
        P("base", "chan", None),
    )
    return jax.shard_map(
        per_device, mesh=mesh, in_specs=in_specs, out_specs=(P(AXES, None), P()), check_vma=False
    )
```

```python
import functools
import math

import jax
import jax.numpy as jnp
import ml_dtypes
import numpy as np
from jax import lax
from jax.experimental import pallas as pl
from jax.experimental.pallas import tpu as pltpu
from jax.sharding import PartitionSpec as P

AXES = ("base", "chan")
N = 2048
DEV = 256
ROWS = 8
CELLS = 256
SLOTS = 256
VCAP = 8
SAMPLES = SLOTS * VCAP
LANES = 128
MSG = 18
GROUP = 4
START_SCALE = 2.0**-11
NORM_LANE = 40
PACK_LIMIT = 64_200_000
F32 = jnp.float32
BF16 = jnp.bfloat16
SMEM = pl.BlockSpec(memory_space=pltpu.SMEM)
VMEM = pl.BlockSpec(memory_space=pltpu.VMEM)
HBM = pl.BlockSpec(memory_space=pltpu.HBM)


def chip_path():
    path = []
    for x in range(4):
        for step_y, y in enumerate(range(4) if x % 2 == 0 else range(3, -1, -1)):
            zs = range(8) if (x * 4 + step_y) % 2 == 0 else range(7, -1, -1)
            path.extend((x, y, z) for z in zs)
    return path


def block_places():
    places = [0] * DEV
    for o, (x, y, z) in enumerate(chip_path()):
        for core in range(2):
            place = (x * 8 + z % 4 * 2 + core) * 8 + y * 2 + z // 4
            places[o if core == 0 else DEV - 1 - o] = place
    return places


PLACES = block_places()
MIRROR = [(PLACES[o], PLACES[DEV - 1 - o]) for o in range(DEV)]
SELF_EDGE = (0, DEV // 2)
MIRROR_EDGE = [
    (PLACES[o], PLACES[DEV // 2 - o if o in SELF_EDGE else DEV - o]) for o in range(DEV)
]


def halves(table):
    high = table.astype(ml_dtypes.bfloat16)
    low = (table - high.astype(np.float64)).astype(ml_dtypes.bfloat16)
    return high, low


def turns(products, modulus):
    angle = 2.0 * np.pi * (np.asarray(products) % modulus) / modulus
    return np.cos(angle), np.sin(angle)


@functools.cache
def tables():
    out = {}
    index = np.arange(DEV)
    for name, rows in (("plain", index), ("placed", np.array(PLACES))):
        cos, sin = turns(rows[:, None] * index[None, :], DEV)
        out[name] = halves(np.concatenate([cos, sin], axis=1))
    small = np.arange(8)
    cos, sin = turns(small[:, None] * index[None, :], N)
    out["turn"] = np.concatenate([cos, sin], axis=0).astype(np.float32)
    cos8, sin8 = turns(small[:, None] * small[None, :], 8)
    eye = np.eye(8)
    cos, sin = np.kron(eye, cos8), np.kron(eye, sin8)
    out["eight_fwd"] = halves(np.block([[cos, sin], [-sin, cos]]))
    out["eight_inv"] = halves(np.block([[cos, -sin], [sin, cos]]))
    row = np.arange(64)
    tile = row % 8 * 8 + row // 8
    place = np.argsort(tile)
    flips = []
    for source in (63 - tile, (64 - tile) % 64):
        one = np.zeros((64, 64))
        one[row, place[source]] = 1.0
        flips.append(np.kron(np.diag([1.0, -1.0]), one))
    out["flip_tile"] = np.concatenate(flips, axis=0).astype(ml_dtypes.bfloat16)
    cell = np.arange(CELLS)
    target = (8 - cell // 32) % 8 * 32 + (32 - cell % 32) % 32
    flip = np.zeros((CELLS, CELLS))
    flip[target, cell] = 1.0
    out["flip_cell"] = flip.astype(ml_dtypes.bfloat16)
    spread = (index[:, None] % 32 == index[None, :] // 8).astype(ml_dtypes.bfloat16)
    out["spread"] = spread
    share = np.zeros((DEV, 8))
    share[: DEV // 2, :4] = 2.0
    share[DEV // 2 :, 1:5] = 2.0
    share[0, 0] = 1.0
    share[DEV // 2, 0] = 1.0
    share = np.repeat(share, ROWS, axis=1)
    out["share"] = np.concatenate([share, share], axis=1).astype(np.float32)
    return out


def split(x):
    high = x.astype(BF16)
    return high, (x - high.astype(F32)).astype(BF16)


def dot(a, b, dims=((1,), (0,))):
    return lax.dot_general(a, b, (dims, ((), ())), preferred_element_type=F32)


def dot3(a, b, dims=((1,), (0,))):
    (ah, al), (bh, bl) = a, b
    rows = ah.shape[0]
    both = dot(jnp.concatenate([ah, al], axis=0), bh, dims)
    return both[:rows] + (both[rows:] + dot(ah, bl, dims))


NT = ((1,), (1,))


def load_pair(high_ref, low_ref):
    return high_ref[...], low_ref[...]


def swap_chunks(x):
    chunk = lax.broadcasted_iota(jnp.int32, (8, LANES), 1) // 32
    blocks = {}
    for part in range(2):
        for a_high in range(2):
            for b_high in range(2):
                source = [
                    x[
                        part * 64 + (a_high * 4 + a) * 8 : part * 64 + (a_high * 4 + a) * 8 + 8,
                        b_high * LANES : (b_high + 1) * LANES,
                    ]
                    for a in range(4)
                ]
                for b in range(4):
                    made = None
                    for a in range(4):
                        shift = (a - b) * 32 % LANES
                        moved = source[a] if shift == 0 else pltpu.roll(source[a], shift, 1)
                        made = moved if made is None else jnp.where(chunk == a, moved, made)
                    blocks[part, b_high * 4 + b, a_high] = made
    rows = [
        jnp.concatenate([blocks[part, b, 0], blocks[part, b, 1]], axis=1)
        for part in range(2)
        for b in range(8)
    ]
    return jnp.concatenate(rows, axis=0)


def fold(x):
    squares = x * x
    total = None
    for i in range(x.shape[0] // 8):
        for j in range(x.shape[1] // LANES):
            piece = squares[i * 8 : i * 8 + 8, j * LANES : (j + 1) * LANES]
            total = piece if total is None else total + piece
    return total


def apply_matrix(spectrum, samples, mask_ref):
    parts = split(spectrum)
    row = lax.broadcasted_iota(jnp.int32, (LANES, 256), 0)
    tile = (row % 8 * 8 + row // 8 % 8).astype(F32)
    total = None
    for m in range(SAMPLES // 256):
        a = samples(m)
        seen = dot3(parts, a, NT)
        weight = mask_ref[m : m + 1, :]
        wanted = mask_ref[8 + m : 9 + m, :]
        kept = jnp.where(tile == wanted, seen * weight, 0.0)
        added = dot3(split(kept), a)
        total = added if total is None else total + added
    return total


def stored_samples(ah_ref, al_ref):
    return lambda m: (ah_ref[pl.ds(m * 256, 256), :], al_ref[pl.ds(m * 256, 256), :])


def pack_edge(grid):
    chunk = lax.broadcasted_iota(jnp.int32, (32, LANES), 1) // 32
    made = grid[:32, :LANES]
    for i in range(1, 4):
        moved = pltpu.roll(grid[i * 32 : i * 32 + 32, :LANES], i * 32, 1)
        made = jnp.where(chunk == i, moved, made)
    return made


def unpack_edge(edge):
    return jnp.concatenate(
        [edge] + [pltpu.roll(edge, LANES - i * 32, 1) for i in range(1, 4)], axis=0
    )


def mirrored(own_ref, other_ref, sent_ref, edge_ref, alone_ref, flip_tile_ref, flip_cell_ref):
    lane = lax.broadcasted_iota(jnp.int32, (LANES, CELLS), 1)
    other = other_ref[...]
    edge = jnp.where(alone_ref[0, 0] > 0, sent_ref[...], edge_ref[...])
    edge = jnp.concatenate([unpack_edge(edge), other[:, LANES:]], axis=1)
    other = jnp.where(lane < 32, edge, other)
    high, low = split(other)
    flips = flip_tile_ref[...]
    turned = dot(jnp.concatenate([flips, flips], axis=1), jnp.concatenate([high, low], axis=0))
    turned = jnp.where(lane % 32 == 0, turned[LANES:], turned[:LANES])
    high, low = split(turned)
    flip = flip_cell_ref[...]
    turned = dot(jnp.concatenate([high, low], axis=0), flip)
    return 0.5 * (own_ref[...] + (turned[:LANES] + turned[LANES:]))


def pack_kernel(image_hbm, interp_hbm, weight_hbm, index_hbm, counts_hbm, th_hbm, tl_hbm, turn_hbm,
                out_hbm, norm_ref, out_ref, image_ref, held, weight_ref, index_ref, counts_ref,
                th_ref, tl_ref, turn_ref, sems):
    pieces = 8
    size = SLOTS // pieces
    pairs = [
        (image_hbm, image_ref), (turn_hbm, turn_ref), (th_hbm, th_ref), (tl_hbm, tl_ref),
        (index_hbm, index_ref), (counts_hbm, counts_ref), (weight_hbm, weight_ref),
    ]
    pairs += [
        (interp_hbm.at[pl.ds(i * size, size)], held.at[pl.ds(i * size, size)])
        for i in range(pieces)
    ]
    copies = [
        pltpu.make_async_copy(source, target, sems.at[i])
        for i, (source, target) in enumerate(pairs)
    ]
    for copy in copies:
        copy.start()
    copies[0].wait()
    copies[1].wait()
    image = image_ref[...]
    x = [image[:, q * 256 : (q + 1) * 256] for q in range(8)]
    squares = None
    for q in range(8):
        both = x[q][:, :LANES] ** 2 + x[q][:, LANES:] ** 2
        squares = both if squares is None else squares + both
    norm_ref[...] = squares
    re, im = [None] * 8, [None] * 8
    for c in range(5):
        cos = [math.cos(2.0 * math.pi * (c * q % 8) / 8) for q in range(8)]
        sin = [math.sin(2.0 * math.pi * (c * q % 8) / 8) for q in range(8)]
        re[c] = sum(x[q] * cos[q] for q in range(1, 8)) + x[0]
        im[c] = jnp.zeros_like(x[0]) if c % 4 == 0 else -sum(x[q] * sin[q] for q in range(1, 8))
        if 0 < c < 4:
            re[8 - c] = re[c]
            im[8 - c] = -im[c]
    turned_re, turned_im = [], []
    for c in range(8):
        cos, sin = turn_ref[c : c + 1, :], turn_ref[8 + c : 9 + c, :]
        turned_re.append(re[c] * cos + im[c] * sin)
        turned_im.append(im[c] * cos - re[c] * sin)
    plain = jnp.concatenate(turned_re + turned_im, axis=0)
    crossed = jnp.concatenate(turned_im + [-v for v in turned_re], axis=0)
    data = split(jnp.concatenate([plain, crossed], axis=1))
    copies[2].wait()
    copies[3].wait()
    columns = dot3(load_pair(th_ref, tl_ref), data, NT)
    out_ref[pl.ds(16, DEV, stride=MSG), :] = columns
    for i in (4, 5, 6):
        copies[i].wait()
    marks = jnp.concatenate(
        [
            weight_ref[...],
            index_ref[...].astype(F32),
            counts_ref[...].astype(F32),
            jnp.zeros((LANES - 10, SLOTS), F32),
        ],
        axis=0,
    )
    out_ref[pl.ds(17, DEV, stride=MSG), :] = marks.T

    def move(group, carry):
        base = pl.multiple_of(group * (GROUP * MSG), 8)
        for m in range(GROUP):
            for tile in range(2):
                out_ref[pl.ds(base + m * MSG + tile * 8, 8), :] = held[
                    group * GROUP + m, :, tile * LANES : (tile + 1) * LANES
                ]
        return carry

    groups = SLOTS // GROUP // pieces
    rows = size * MSG
    sent = []
    for i in range(pieces):
        copies[7 + i].wait()
        lax.fori_loop(i * groups, (i + 1) * groups, move, 0, unroll=2)
        part = pl.ds(i * rows, rows)
        sent.append(
            pltpu.make_async_copy(out_ref.at[part], out_hbm.at[part], sems.at[15 + i])
        )
        sent[-1].start()
    for copy in sent:
        copy.wait()


def first_kernel(got_ref, th_ref, tl_ref, turn_ref, eh_ref, el_ref, spread_ref,
                 out_ref, edge_ref, ah_ref, al_ref, mask_ref):
    def samples(m):
        slots = [
            jnp.concatenate(
                [got_ref[pl.ds(slot * MSG + t * 8, 8), :] for t in range(2)], axis=1
            )
            for slot in range(m * 32, m * 32 + 32)
        ]
        high, low = split(jnp.concatenate(slots, axis=0))
        ah_ref[pl.ds(m * 256, 256), :] = high
        al_ref[pl.ds(m * 256, 256), :] = low
        return high, low

    marks = got_ref[pl.ds(17, DEV, stride=MSG), :].T[:16]
    chunk = lax.broadcasted_iota(jnp.int32, (16, SLOTS), 1) // 32
    stacked = jnp.concatenate([jnp.where(chunk == m, marks, 0.0) for m in range(8)], axis=0)
    high, low = split(stacked)
    lowest = (stacked - high.astype(F32) - low.astype(F32)).astype(BF16)
    spread = spread_ref[...]
    spread_marks = dot(high, spread) + (dot(low, spread) + dot(lowest, spread))
    sample = lax.broadcasted_iota(jnp.int32, (8, 256), 1) % 8
    row = lax.broadcasted_iota(jnp.int32, (8, 256), 0)
    for m in range(8):
        block = spread_marks[m * 16 : m * 16 + 16]
        weight = jnp.sum(jnp.where(sample == row, block[:8], 0.0), axis=0, keepdims=True)
        live = sample[:1].astype(F32) < block[9:10]
        mask_ref[m : m + 1, :] = jnp.where(live, weight, 0.0)
        mask_ref[8 + m : 9 + m, :] = block[8:9]

    columns = got_ref[pl.ds(16, DEV, stride=MSG), :].T
    both = dot3(split(columns), load_pair(th_ref, tl_ref))
    by_cos, by_sin = both[:, :DEV], both[:, DEV:]
    re = (by_cos[:64] + by_sin[64:]).reshape(8, 8, DEV)
    im = (by_cos[64:] - by_sin[:64]).reshape(8, 8, DEV)
    scale = START_SCALE / N
    cos, sin = turn_ref[:8, :] * scale, turn_ref[8:, :] * scale
    turned = jnp.concatenate([re * cos + im * sin, im * cos - re * sin], axis=0)
    spectrum = dot3(load_pair(eh_ref, el_ref), split(turned.reshape(LANES, DEV)))
    grid = apply_matrix(swap_chunks(spectrum), samples, mask_ref)
    out_ref[...] = grid
    edge_ref[...] = pack_edge(grid)


def next_kernel(own_ref, other_ref, sent_ref, edge_ref, alone_ref, ah_ref, al_ref, mask_ref, ft_ref, fc_ref,
                out_ref, edge_out_ref, norm_ref):
    spectrum = mirrored(own_ref, other_ref, sent_ref, edge_ref, alone_ref, ft_ref, fc_ref)
    norm_ref[...] = fold(spectrum)
    grid = apply_matrix(spectrum, stored_samples(ah_ref, al_ref), mask_ref)
    out_ref[...] = grid
    edge_out_ref[...] = pack_edge(grid)


def send_kernel(own_ref, other_ref, sent_ref, edge_ref, alone_ref, n0_ref, n1_ref, n2_ref, ft_ref, fc_ref,
                th_ref, tl_ref, turn_ref, eh_ref, el_ref, out_ref):
    spectrum = mirrored(own_ref, other_ref, sent_ref, edge_ref, alone_ref, ft_ref, fc_ref)
    norms = [jnp.sum(n) for n in (n0_ref[...], n1_ref[...], n2_ref[...], fold(spectrum))]
    data = dot3(load_pair(eh_ref, el_ref), split(swap_chunks(spectrum)))
    re = data[:64].reshape(8, 8, DEV)
    im = data[64:].reshape(8, 8, DEV)
    cos, sin = turn_ref[:8, :] * (1.0 / N), turn_ref[8:, :] * (1.0 / N)
    turned_re = (re * cos - im * sin).reshape(64, DEV)
    turned_im = (im * cos + re * sin).reshape(64, DEV)
    plain = jnp.concatenate([turned_re, turned_im], axis=0)
    crossed = jnp.concatenate([-turned_im, turned_re], axis=0)
    data = split(jnp.concatenate([plain, crossed], axis=1))
    out = dot3(load_pair(th_ref, tl_ref), data, NT)
    lane = lax.broadcasted_iota(jnp.int32, (DEV, LANES), 1)
    for i in range(4):
        out = jnp.where(lane == NORM_LANE + i, norms[i], out)
    out_ref[...] = out


def last_kernel(got_ref, share_ref, th_ref, tl_ref, turn_ref, image_ref, found_ref):
    got = got_ref[...]
    totals = jnp.sum(got, axis=0, keepdims=True)
    norms = [jnp.sqrt(totals[:, NORM_LANE + i : NORM_LANE + i + 1]) for i in range(4)]
    first = norms[1] / (norms[0] * START_SCALE)
    rest = [norms[2] / norms[1], norms[3] / norms[2]]
    lane = lax.broadcasted_iota(jnp.int32, (1, 3), 1)
    found_ref[...] = jnp.where(lane == 0, first, jnp.where(lane == 1, rest[0], rest[1]))
    both = dot3(split((got * share_ref[...]).T), load_pair(th_ref, tl_ref))
    by_cos, by_sin = both[:, :DEV], both[:, DEV:]
    factor = float(N) / norms[3]
    re, im = [], []
    for c in range(5):
        here, there = slice(c * 8, c * 8 + 8), slice(64 + c * 8, 72 + c * 8)
        r = by_cos[here] - by_sin[there]
        i = by_cos[there] + by_sin[here]
        cos, sin = turn_ref[c : c + 1, :] * factor, turn_ref[8 + c : 9 + c, :] * factor
        re.append(r * cos - i * sin)
        im.append(i * cos + r * sin)
    for j in range(8):
        total = re[0]
        for c in range(1, 5):
            cos = math.cos(2.0 * math.pi * (c * j % 8) / 8)
            sin = math.sin(2.0 * math.pi * (c * j % 8) / 8)
            total = total + re[c] * cos - im[c] * sin
        image_ref[:, j * 256 : (j + 1) * 256] = total


def call(kernel, outs, in_specs, flops, moved, scratch=(), limit=24 * 2**20, out_specs=None):
    return pl.pallas_call(
        kernel,
        out_shape=tuple(jax.ShapeDtypeStruct(s, t) for s, t in outs),
        in_specs=in_specs,
        out_specs=out_specs or tuple(VMEM for _ in outs),
        scratch_shapes=list(scratch),
        compiler_params=pltpu.CompilerParams(vmem_limit_bytes=limit),
        cost_estimate=pl.CostEstimate(flops=flops, bytes_accessed=moved, transcendentals=0),
    )


def exchange(message):
    rows = message.shape[0]
    out = lax.all_to_all(
        message.reshape(rows, 1, LANES), AXES, 0, 0, tiled=True, axis_index_groups=[PLACES]
    )
    return out.reshape(rows, LANES)


def mirror_exchange(grid, edge, alone):
    got = lax.ppermute(edge, AXES, MIRROR_EDGE)
    other = lax.ppermute(grid, AXES, MIRROR)
    return grid, other, edge, got, alone


def per_device(image0, interp, vis_weight, counts, tile_index):
    t = {
        k: tuple(jnp.asarray(a) for a in v) if isinstance(v, tuple) else jnp.asarray(v)
        for k, v in tables().items()
    }
    pack = call(
        pack_kernel,
        [((DEV * MSG, LANES), F32), ((8, LANES), F32)],
        [HBM] * 8,
        200_000_000,
        5_000_000,
        scratch=[
            pltpu.VMEM((DEV * MSG, LANES), F32),
            pltpu.VMEM((ROWS, N), F32),
            pltpu.VMEM((SLOTS, VCAP, CELLS), F32),
            pltpu.VMEM((VCAP, SLOTS), F32),
            pltpu.VMEM((1, SLOTS), jnp.int32),
            pltpu.VMEM((1, SLOTS), jnp.int32),
            pltpu.VMEM((DEV, 2 * DEV), BF16),
            pltpu.VMEM((DEV, 2 * DEV), BF16),
            pltpu.VMEM((16, DEV), F32),
            pltpu.SemaphoreType.DMA((23,)),
        ],
        limit=PACK_LIMIT,
        out_specs=(HBM, VMEM),
    )
    message, n0 = pack(
        image0,
        interp.reshape(SLOTS, VCAP, CELLS),
        vis_weight.reshape(SLOTS, VCAP).T,
        tile_index.reshape(1, SLOTS),
        counts.reshape(1, SLOTS),
        *t["plain"],
        t["turn"],
    )
    got = exchange(message)
    first = call(
        first_kernel,
        [
            ((LANES, CELLS), F32),
            ((32, LANES), F32),
            ((SAMPLES, CELLS), BF16),
            ((SAMPLES, CELLS), BF16),
            ((16, 256), F32),
        ],
        [VMEM] * 7,
        1_000_000_000,
        5_000_000,
    )
    grid, edge, a_high, a_low, mask = first(
        got, *t["placed"], t["turn"], *t["eight_fwd"], t["spread"]
    )
    place = lax.axis_index(AXES)
    alone = (place == PLACES[SELF_EDGE[0]]) | (place == PLACES[SELF_EDGE[1]])
    alone = alone.astype(jnp.int32).reshape(1, 1)
    norms = [n0]
    follow = call(
        next_kernel,
        [((LANES, CELLS), F32), ((32, LANES), F32), ((8, LANES), F32)],
        [VMEM] * 4 + [SMEM] + [VMEM] * 5,
        1_000_000_000,
        3_000_000,
    )
    for _ in range(2):
        blocks = mirror_exchange(grid, edge, alone)
        grid, edge, norm = follow(
            *blocks, a_high, a_low, mask, t["flip_tile"], t["flip_cell"]
        )
        norms.append(norm)
    blocks = mirror_exchange(grid, edge, alone)
    send = call(
        send_kernel, [((DEV, LANES), F32)], [VMEM] * 4 + [SMEM] + [VMEM] * 10, 300_000_000, 1_500_000
    )
    (message,) = send(
        *blocks, *norms, t["flip_tile"], t["flip_cell"],
        *t["placed"], t["turn"], *t["eight_inv"],
    )
    got = exchange(message)
    last = call(
        last_kernel,
        [((ROWS, N), F32), ((1, 3), F32)],
        [VMEM] * 5,
        200_000_000,
        1_500_000,
    )
    image, found = last(got, t["share"], *t["plain"], t["turn"])
    return image, found.reshape(3)


def solution(mesh):
    in_specs = (
        P(AXES, None),
        P("base", "chan", None, None, None),
        P("base", "chan", None, None),
        P("base", "chan", None),
        P("base", "chan", None),
    )
    return jax.shard_map(
        per_device, mesh=mesh, in_specs=in_specs, out_specs=(P(AXES, None), P()), check_vma=False
    )
```

```python
import functools
import math

import jax
import jax.numpy as jnp
import ml_dtypes
import numpy as np
from jax import lax
from jax.experimental import pallas as pl
from jax.experimental.pallas import tpu as pltpu
from jax.sharding import PartitionSpec as P

AXES = ("base", "chan")
N = 2048
DEV = 256
ROWS = 8
CELLS = 256
SLOTS = 256
VCAP = 8
SAMPLES = SLOTS * VCAP
LANES = 128
MSG = 18
GROUP = 4
START_SCALE = 2.0**-11
NORM_LANE = 40
PACK_LIMIT = 64_200_000
F32 = jnp.float32
BF16 = jnp.bfloat16
SMEM = pl.BlockSpec(memory_space=pltpu.SMEM)
VMEM = pl.BlockSpec(memory_space=pltpu.VMEM)
HBM = pl.BlockSpec(memory_space=pltpu.HBM)


def chip_path():
    path = []
    for z in range(8):
        plane = []
        for y in range(4):
            xs = range(4) if y % 2 == 0 else range(3, -1, -1)
            plane.extend((x, y, z) for x in xs)
        path.extend(plane if z % 2 == 0 else plane[::-1])
    return path


def block_places():
    places = [0] * DEV
    for o, (x, y, z) in enumerate(chip_path()):
        for core in range(2):
            place = (x * 8 + z % 4 * 2 + core) * 8 + y * 2 + z // 4
            places[o if core == 0 else DEV - 1 - o] = place
    return places


PLACES = block_places()
MIRROR = [(PLACES[o], PLACES[DEV - 1 - o]) for o in range(DEV)]
SELF_EDGE = (0, DEV // 2)
MIRROR_EDGE = [
    (PLACES[o], PLACES[DEV // 2 - o if o in SELF_EDGE else DEV - o]) for o in range(DEV)
]


def halves(table):
    high = table.astype(ml_dtypes.bfloat16)
    low = (table - high.astype(np.float64)).astype(ml_dtypes.bfloat16)
    return high, low


def turns(products, modulus):
    angle = 2.0 * np.pi * (np.asarray(products) % modulus) / modulus
    return np.cos(angle), np.sin(angle)


@functools.cache
def tables():
    out = {}
    index = np.arange(DEV)
    for name, rows in (("plain", index), ("placed", np.array(PLACES))):
        cos, sin = turns(rows[:, None] * index[None, :], DEV)
        out[name] = halves(np.concatenate([cos, sin], axis=1))
    few = np.arange(16)
    coarse = turns(few[:, None] * index[None, :], 16)
    fine = turns(few[:, None] * index[None, :], DEV)
    small = np.arange(8)
    cos, sin = turns(small[:, None] * index[None, :], N)
    out["turn"] = np.concatenate([cos, sin], axis=0).astype(np.float32)
    out["start"] = np.concatenate([cos, sin, *fine, *coarse], axis=0).astype(np.float32)
    cos8, sin8 = turns(small[:, None] * small[None, :], 8)
    eye = np.eye(8)
    cos, sin = np.kron(eye, cos8), np.kron(eye, sin8)
    out["eight_fwd"] = halves(np.block([[cos, sin], [-sin, cos]]))
    out["eight_inv"] = halves(np.block([[cos, -sin], [sin, cos]]))
    row = np.arange(64)
    tile = row % 8 * 8 + row // 8
    place = np.argsort(tile)
    flips = []
    for source in (63 - tile, (64 - tile) % 64):
        one = np.zeros((64, 64))
        one[row, place[source]] = 1.0
        flips.append(np.kron(np.diag([1.0, -1.0]), one))
    out["flip_tile"] = np.concatenate(flips, axis=0).astype(ml_dtypes.bfloat16)
    cell = np.arange(CELLS)
    target = (8 - cell // 32) % 8 * 32 + (32 - cell % 32) % 32
    flip = np.zeros((CELLS, CELLS))
    flip[target, cell] = 1.0
    out["flip_cell"] = flip.astype(ml_dtypes.bfloat16)
    spread = (index[:, None] % 32 == index[None, :] // 8).astype(ml_dtypes.bfloat16)
    out["spread"] = spread
    share = np.zeros((DEV, 8))
    share[: DEV // 2, :4] = 2.0
    share[DEV // 2 :, 1:5] = 2.0
    share[0, 0] = 1.0
    share[DEV // 2, 0] = 1.0
    share = np.repeat(share, ROWS, axis=1)
    out["share"] = np.concatenate([share, share], axis=1).astype(np.float32)
    return out


def split(x):
    high = x.astype(BF16)
    return high, (x - high.astype(F32)).astype(BF16)


def dot(a, b, dims=((1,), (0,))):
    return lax.dot_general(a, b, (dims, ((), ())), preferred_element_type=F32)


def dot3(a, b, dims=((1,), (0,))):
    (ah, al), (bh, bl) = a, b
    rows = ah.shape[0]
    both = dot(jnp.concatenate([ah, al], axis=0), bh, dims)
    return both[:rows] + (both[rows:] + dot(ah, bl, dims))


NT = ((1,), (1,))


def load_pair(high_ref, low_ref):
    return high_ref[...], low_ref[...]


def swap_chunks(x):
    chunk = lax.broadcasted_iota(jnp.int32, (8, LANES), 1) // 32
    blocks = {}
    for part in range(2):
        for a_high in range(2):
            for b_high in range(2):
                source = [
                    x[
                        part * 64 + (a_high * 4 + a) * 8 : part * 64 + (a_high * 4 + a) * 8 + 8,
                        b_high * LANES : (b_high + 1) * LANES,
                    ]
                    for a in range(4)
                ]
                for b in range(4):
                    made = None
                    for a in range(4):
                        shift = (a - b) * 32 % LANES
                        moved = source[a] if shift == 0 else pltpu.roll(source[a], shift, 1)
                        made = moved if made is None else jnp.where(chunk == a, moved, made)
                    blocks[part, b_high * 4 + b, a_high] = made
    rows = [
        jnp.concatenate([blocks[part, b, 0], blocks[part, b, 1]], axis=1)
        for part in range(2)
        for b in range(8)
    ]
    return jnp.concatenate(rows, axis=0)


def fold(x):
    squares = x * x
    total = None
    for i in range(x.shape[0] // 8):
        for j in range(x.shape[1] // LANES):
            piece = squares[i * 8 : i * 8 + 8, j * LANES : (j + 1) * LANES]
            total = piece if total is None else total + piece
    return total


def apply_matrix(spectrum, samples, mask_ref):
    parts = split(spectrum)
    row = lax.broadcasted_iota(jnp.int32, (LANES, 256), 0)
    tile = (row % 8 * 8 + row // 8 % 8).astype(F32)
    total = None
    for m in range(SAMPLES // 256):
        a = samples(m)
        seen = dot3(parts, a, NT)
        weight = mask_ref[m : m + 1, :]
        wanted = mask_ref[8 + m : 9 + m, :]
        kept = jnp.where(tile == wanted, seen * weight, 0.0)
        added = dot3(split(kept), a)
        total = added if total is None else total + added
    return total


def stored_samples(ah_ref, al_ref):
    return lambda m: (ah_ref[pl.ds(m * 256, 256), :], al_ref[pl.ds(m * 256, 256), :])


def pack_edge(grid):
    chunk = lax.broadcasted_iota(jnp.int32, (32, LANES), 1) // 32
    made = grid[:32, :LANES]
    for i in range(1, 4):
        moved = pltpu.roll(grid[i * 32 : i * 32 + 32, :LANES], i * 32, 1)
        made = jnp.where(chunk == i, moved, made)
    return made


def unpack_edge(edge):
    return jnp.concatenate(
        [edge] + [pltpu.roll(edge, LANES - i * 32, 1) for i in range(1, 4)], axis=0
    )


def mirrored(own_ref, other_ref, sent_ref, edge_ref, alone_ref, flip_tile_ref, flip_cell_ref):
    lane = lax.broadcasted_iota(jnp.int32, (LANES, CELLS), 1)
    other = other_ref[...]
    edge = jnp.where(alone_ref[0, 0] > 0, sent_ref[...], edge_ref[...])
    edge = jnp.concatenate([unpack_edge(edge), other[:, LANES:]], axis=1)
    other = jnp.where(lane < 32, edge, other)
    high, low = split(other)
    flips = flip_tile_ref[...]
    turned = dot(jnp.concatenate([flips, flips], axis=1), jnp.concatenate([high, low], axis=0))
    turned = jnp.where(lane % 32 == 0, turned[LANES:], turned[:LANES])
    high, low = split(turned)
    flip = flip_cell_ref[...]
    turned = dot(jnp.concatenate([high, low], axis=0), flip)
    return 0.5 * (own_ref[...] + (turned[:LANES] + turned[LANES:]))


def pack_kernel(image_hbm, interp_hbm, weight_hbm, index_hbm, counts_hbm, turn_hbm,
                out_hbm, out_ref, image_ref, held, weight_ref, index_ref, counts_ref,
                turn_ref, table_ref, sems):
    pieces = 8
    size = SLOTS // pieces
    pairs = [
        (turn_hbm, turn_ref), (image_hbm, image_ref),
        (index_hbm, index_ref), (counts_hbm, counts_ref), (weight_hbm, weight_ref),
    ]
    pairs += [
        (interp_hbm.at[pl.ds(i * size, size)], held.at[pl.ds(i * size, size)])
        for i in range(pieces)
    ]
    copies = [
        pltpu.make_async_copy(source, target, sems.at[i])
        for i, (source, target) in enumerate(pairs)
    ]
    for copy in copies:
        copy.start()
    copies[0].wait()
    cos_b, sin_b = turn_ref[16:32, :], turn_ref[32:48, :]
    for a in range(16):
        cos_a, sin_a = turn_ref[48 + a : 49 + a, :], turn_ref[64 + a : 65 + a, :]
        rows = slice(a * 16, a * 16 + 16)
        table_ref[0, rows, :DEV], table_ref[1, rows, :DEV] = split(cos_a * cos_b - sin_a * sin_b)
        table_ref[0, rows, DEV:], table_ref[1, rows, DEV:] = split(sin_a * cos_b + cos_a * sin_b)
    copies[1].wait()
    image = image_ref[...]
    x = [image[:, q * 256 : (q + 1) * 256] for q in range(8)]
    re, im = [None] * 8, [None] * 8
    for c in range(5):
        cos = [math.cos(2.0 * math.pi * (c * q % 8) / 8) for q in range(8)]
        sin = [math.sin(2.0 * math.pi * (c * q % 8) / 8) for q in range(8)]
        re[c] = sum(x[q] * cos[q] for q in range(1, 8)) + x[0]
        im[c] = jnp.zeros_like(x[0]) if c % 4 == 0 else -sum(x[q] * sin[q] for q in range(1, 8))
        if 0 < c < 4:
            re[8 - c] = re[c]
            im[8 - c] = -im[c]
    turned_re, turned_im = [], []
    for c in range(8):
        cos, sin = turn_ref[c : c + 1, :], turn_ref[8 + c : 9 + c, :]
        turned_re.append(re[c] * cos + im[c] * sin)
        turned_im.append(im[c] * cos - re[c] * sin)
    plain = jnp.concatenate(turned_re + turned_im, axis=0)
    crossed = jnp.concatenate(turned_im + [-v for v in turned_re], axis=0)
    data = split(jnp.concatenate([plain, crossed], axis=1))
    columns = dot3((table_ref[0], table_ref[1]), data, NT)
    out_ref[pl.ds(16, DEV, stride=MSG), :] = columns
    for i in (2, 3, 4):
        copies[i].wait()
    marks = jnp.concatenate(
        [
            weight_ref[...],
            index_ref[...].astype(F32),
            counts_ref[...].astype(F32),
            jnp.zeros((LANES - 10, SLOTS), F32),
        ],
        axis=0,
    )
    out_ref[pl.ds(17, DEV, stride=MSG), :] = marks.T

    def move(group, carry):
        base = pl.multiple_of(group * (GROUP * MSG), 8)
        for m in range(GROUP):
            for tile in range(2):
                out_ref[pl.ds(base + m * MSG + tile * 8, 8), :] = held[
                    group * GROUP + m, :, tile * LANES : (tile + 1) * LANES
                ]
        return carry

    groups = SLOTS // GROUP // pieces
    rows = size * MSG
    sent = []
    for i in range(pieces):
        copies[5 + i].wait()
        lax.fori_loop(i * groups, (i + 1) * groups, move, 0, unroll=2)
        part = pl.ds(i * rows, rows)
        sent.append(
            pltpu.make_async_copy(out_ref.at[part], out_hbm.at[part], sems.at[13 + i])
        )
        sent[-1].start()
    for copy in sent:
        copy.wait()


def first_kernel(got_ref, th_ref, tl_ref, turn_ref, eh_ref, el_ref, spread_ref,
                 out_ref, edge_ref, ah_ref, al_ref, mask_ref, norm_ref):
    def samples(m):
        slots = [
            jnp.concatenate(
                [got_ref[pl.ds(slot * MSG + t * 8, 8), :] for t in range(2)], axis=1
            )
            for slot in range(m * 32, m * 32 + 32)
        ]
        high, low = split(jnp.concatenate(slots, axis=0))
        ah_ref[pl.ds(m * 256, 256), :] = high
        al_ref[pl.ds(m * 256, 256), :] = low
        return high, low

    marks = got_ref[pl.ds(17, DEV, stride=MSG), :].T[:16]
    chunk = lax.broadcasted_iota(jnp.int32, (16, SLOTS), 1) // 32
    stacked = jnp.concatenate([jnp.where(chunk == m, marks, 0.0) for m in range(8)], axis=0)
    high, low = split(stacked)
    lowest = (stacked - high.astype(F32) - low.astype(F32)).astype(BF16)
    spread = spread_ref[...]
    spread_marks = dot(high, spread) + (dot(low, spread) + dot(lowest, spread))
    sample = lax.broadcasted_iota(jnp.int32, (8, 256), 1) % 8
    row = lax.broadcasted_iota(jnp.int32, (8, 256), 0)
    for m in range(8):
        block = spread_marks[m * 16 : m * 16 + 16]
        weight = jnp.sum(jnp.where(sample == row, block[:8], 0.0), axis=0, keepdims=True)
        live = sample[:1].astype(F32) < block[9:10]
        mask_ref[m : m + 1, :] = jnp.where(live, weight, 0.0)
        mask_ref[8 + m : 9 + m, :] = block[8:9]

    columns = got_ref[pl.ds(16, DEV, stride=MSG), :].T
    both = dot3(split(columns), load_pair(th_ref, tl_ref))
    by_cos, by_sin = both[:, :DEV], both[:, DEV:]
    re = (by_cos[:64] + by_sin[64:]).reshape(8, 8, DEV)
    im = (by_cos[64:] - by_sin[:64]).reshape(8, 8, DEV)
    scale = START_SCALE / N
    cos, sin = turn_ref[:8, :] * scale, turn_ref[8:, :] * scale
    turned = jnp.concatenate([re * cos + im * sin, im * cos - re * sin], axis=0)
    spectrum = dot3(load_pair(eh_ref, el_ref), split(turned.reshape(LANES, DEV)))
    spectrum = swap_chunks(spectrum)
    norm_ref[...] = fold(spectrum)
    grid = apply_matrix(spectrum, samples, mask_ref)
    out_ref[...] = grid
    edge_ref[...] = pack_edge(grid)


def next_kernel(own_ref, other_ref, sent_ref, edge_ref, alone_ref, ah_ref, al_ref, mask_ref, ft_ref, fc_ref,
                out_ref, edge_out_ref, norm_ref):
    spectrum = mirrored(own_ref, other_ref, sent_ref, edge_ref, alone_ref, ft_ref, fc_ref)
    norm_ref[...] = fold(spectrum)
    grid = apply_matrix(spectrum, stored_samples(ah_ref, al_ref), mask_ref)
    out_ref[...] = grid
    edge_out_ref[...] = pack_edge(grid)


def send_kernel(own_ref, other_ref, sent_ref, edge_ref, alone_ref, n0_ref, n1_ref, n2_ref, ft_ref, fc_ref,
                th_ref, tl_ref, turn_ref, eh_ref, el_ref, out_ref):
    spectrum = mirrored(own_ref, other_ref, sent_ref, edge_ref, alone_ref, ft_ref, fc_ref)
    norms = [jnp.sum(n) for n in (n0_ref[...], n1_ref[...], n2_ref[...], fold(spectrum))]
    data = dot3(load_pair(eh_ref, el_ref), split(swap_chunks(spectrum)))
    re = data[:64].reshape(8, 8, DEV)
    im = data[64:].reshape(8, 8, DEV)
    cos, sin = turn_ref[:8, :] * (1.0 / N), turn_ref[8:, :] * (1.0 / N)
    turned_re = (re * cos - im * sin).reshape(64, DEV)
    turned_im = (im * cos + re * sin).reshape(64, DEV)
    plain = jnp.concatenate([turned_re, turned_im], axis=0)
    crossed = jnp.concatenate([-turned_im, turned_re], axis=0)
    data = split(jnp.concatenate([plain, crossed], axis=1))
    out = dot3(load_pair(th_ref, tl_ref), data, NT)
    lane = lax.broadcasted_iota(jnp.int32, (DEV, LANES), 1)
    for i in range(4):
        out = jnp.where(lane == NORM_LANE + i, norms[i], out)
    out_ref[...] = out


def last_kernel(got_ref, share_ref, th_ref, tl_ref, turn_ref, image_ref, found_ref):
    got = got_ref[...]
    totals = jnp.sum(got, axis=0, keepdims=True)
    norms = [jnp.sqrt(totals[:, NORM_LANE + i : NORM_LANE + i + 1]) for i in range(4)]
    first = norms[1] / norms[0]
    rest = [norms[2] / norms[1], norms[3] / norms[2]]
    lane = lax.broadcasted_iota(jnp.int32, (1, 3), 1)
    found_ref[...] = jnp.where(lane == 0, first, jnp.where(lane == 1, rest[0], rest[1]))
    both = dot3(split((got * share_ref[...]).T), load_pair(th_ref, tl_ref))
    by_cos, by_sin = both[:, :DEV], both[:, DEV:]
    factor = float(N) / norms[3]
    re, im = [], []
    for c in range(5):
        here, there = slice(c * 8, c * 8 + 8), slice(64 + c * 8, 72 + c * 8)
        r = by_cos[here] - by_sin[there]
        i = by_cos[there] + by_sin[here]
        cos, sin = turn_ref[c : c + 1, :] * factor, turn_ref[8 + c : 9 + c, :] * factor
        re.append(r * cos - i * sin)
        im.append(i * cos + r * sin)
    for j in range(8):
        total = re[0]
        for c in range(1, 5):
            cos = math.cos(2.0 * math.pi * (c * j % 8) / 8)
            sin = math.sin(2.0 * math.pi * (c * j % 8) / 8)
            total = total + re[c] * cos - im[c] * sin
        image_ref[:, j * 256 : (j + 1) * 256] = total


def call(kernel, outs, in_specs, flops, moved, scratch=(), limit=24 * 2**20, out_specs=None):
    return pl.pallas_call(
        kernel,
        out_shape=tuple(jax.ShapeDtypeStruct(s, t) for s, t in outs),
        in_specs=in_specs,
        out_specs=out_specs or tuple(VMEM for _ in outs),
        scratch_shapes=list(scratch),
        compiler_params=pltpu.CompilerParams(vmem_limit_bytes=limit),
        cost_estimate=pl.CostEstimate(flops=flops, bytes_accessed=moved, transcendentals=0),
    )


def exchange(message):
    rows = message.shape[0]
    out = lax.all_to_all(
        message.reshape(rows, 1, LANES), AXES, 0, 0, tiled=True, axis_index_groups=[PLACES]
    )
    return out.reshape(rows, LANES)


def mirror_exchange(grid, edge, alone):
    got = lax.ppermute(edge, AXES, MIRROR_EDGE)
    other = lax.ppermute(grid, AXES, MIRROR)
    return grid, other, edge, got, alone


def per_device(image0, interp, vis_weight, counts, tile_index):
    t = {
        k: tuple(jnp.asarray(a) for a in v) if isinstance(v, tuple) else jnp.asarray(v)
        for k, v in tables().items()
    }
    pack = call(
        pack_kernel,
        [((DEV * MSG, LANES), F32)],
        [HBM] * 6,
        200_000_000,
        5_000_000,
        scratch=[
            pltpu.VMEM((DEV * MSG, LANES), F32),
            pltpu.VMEM((ROWS, N), F32),
            pltpu.VMEM((SLOTS, VCAP, CELLS), F32),
            pltpu.VMEM((VCAP, SLOTS), F32),
            pltpu.VMEM((1, SLOTS), jnp.int32),
            pltpu.VMEM((1, SLOTS), jnp.int32),
            pltpu.VMEM((80, DEV), F32),
            pltpu.VMEM((2, DEV, 2 * DEV), BF16),
            pltpu.SemaphoreType.DMA((21,)),
        ],
        limit=PACK_LIMIT,
        out_specs=(HBM,),
    )
    (message,) = pack(
        image0,
        interp.reshape(SLOTS, VCAP, CELLS),
        vis_weight.reshape(SLOTS, VCAP).T,
        tile_index.reshape(1, SLOTS),
        counts.reshape(1, SLOTS),
        t["start"],
    )
    got = exchange(message)
    first = call(
        first_kernel,
        [
            ((LANES, CELLS), F32),
            ((32, LANES), F32),
            ((SAMPLES, CELLS), BF16),
            ((SAMPLES, CELLS), BF16),
            ((16, 256), F32),
            ((8, LANES), F32),
        ],
        [VMEM] * 7,
        1_000_000_000,
        5_000_000,
    )
    grid, edge, a_high, a_low, mask, n0 = first(
        got, *t["placed"], t["turn"], *t["eight_fwd"], t["spread"]
    )
    place = lax.axis_index(AXES)
    alone = (place == PLACES[SELF_EDGE[0]]) | (place == PLACES[SELF_EDGE[1]])
    alone = alone.astype(jnp.int32).reshape(1, 1)
    norms = [n0]
    follow = call(
        next_kernel,
        [((LANES, CELLS), F32), ((32, LANES), F32), ((8, LANES), F32)],
        [VMEM] * 4 + [SMEM] + [VMEM] * 5,
        1_000_000_000,
        3_000_000,
    )
    for _ in range(2):
        blocks = mirror_exchange(grid, edge, alone)
        grid, edge, norm = follow(
            *blocks, a_high, a_low, mask, t["flip_tile"], t["flip_cell"]
        )
        norms.append(norm)
    blocks = mirror_exchange(grid, edge, alone)
    send = call(
        send_kernel, [((DEV, LANES), F32)], [VMEM] * 4 + [SMEM] + [VMEM] * 10, 300_000_000, 1_500_000
    )
    (message,) = send(
        *blocks, *norms, t["flip_tile"], t["flip_cell"],
        *t["placed"], t["turn"], *t["eight_inv"],
    )
    got = exchange(message)
    last = call(
        last_kernel,
        [((ROWS, N), F32), ((1, 3), F32)],
        [VMEM] * 5,
        200_000_000,
        1_500_000,
    )
    image, found = last(got, t["share"], *t["plain"], t["turn"])
    return image, found.reshape(3)


def solution(mesh):
    in_specs = (
        P(AXES, None),
        P("base", "chan", None, None, None),
        P("base", "chan", None, None),
        P("base", "chan", None),
        P("base", "chan", None),
    )
    return jax.shard_map(
        per_device, mesh=mesh, in_specs=in_specs, out_specs=(P(AXES, None), P()), check_vma=False
    )
```

```python
import functools
import math

import jax
import jax.numpy as jnp
import ml_dtypes
import numpy as np
from jax import lax
from jax.experimental import pallas as pl
from jax.experimental.pallas import tpu as pltpu
from jax.sharding import PartitionSpec as P

AXES = ("base", "chan")
N = 2048
DEV = 256
ROWS = 8
CELLS = 256
SLOTS = 256
VCAP = 8
SAMPLES = SLOTS * VCAP
LANES = 128
MSG = 17
MARK_LANE = 40
GROUP = 8
START_SCALE = 2.0**-11
NORM_LANE = 40
PACK_LIMIT = 64_200_000
F32 = jnp.float32
BF16 = jnp.bfloat16
SMEM = pl.BlockSpec(memory_space=pltpu.SMEM)
VMEM = pl.BlockSpec(memory_space=pltpu.VMEM)
HBM = pl.BlockSpec(memory_space=pltpu.HBM)


def chip_path():
    path = []
    for z in range(8):
        plane = []
        for y in range(4):
            xs = range(4) if y % 2 == 0 else range(3, -1, -1)
            plane.extend((x, y, z) for x in xs)
        path.extend(plane if z % 2 == 0 else plane[::-1])
    return path


def block_places():
    places = [0] * DEV
    for o, (x, y, z) in enumerate(chip_path()):
        for core in range(2):
            place = (x * 8 + z % 4 * 2 + core) * 8 + y * 2 + z // 4
            places[o if core == 0 else DEV - 1 - o] = place
    return places


PLACES = block_places()
MIRROR = [(PLACES[o], PLACES[DEV - 1 - o]) for o in range(DEV)]
SELF_EDGE = (0, DEV // 2)
MIRROR_EDGE = [
    (PLACES[o], PLACES[DEV // 2 - o if o in SELF_EDGE else DEV - o]) for o in range(DEV)
]


def halves(table):
    high = table.astype(ml_dtypes.bfloat16)
    low = (table - high.astype(np.float64)).astype(ml_dtypes.bfloat16)
    return high, low


def turns(products, modulus):
    angle = 2.0 * np.pi * (np.asarray(products) % modulus) / modulus
    return np.cos(angle), np.sin(angle)


@functools.cache
def tables():
    out = {}
    index = np.arange(DEV)
    for name, rows in (("plain", index), ("placed", np.array(PLACES))):
        cos, sin = turns(rows[:, None] * index[None, :], DEV)
        out[name] = halves(np.concatenate([cos, sin], axis=1))
    few = np.arange(16)
    coarse = turns(few[:, None] * index[None, :], 16)
    fine = turns(few[:, None] * index[None, :], DEV)
    small = np.arange(8)
    cos, sin = turns(small[:, None] * index[None, :], N)
    out["turn"] = np.concatenate([cos, sin], axis=0).astype(np.float32)
    out["start"] = np.concatenate([cos, sin, *fine, *coarse], axis=0).astype(np.float32)
    cos8, sin8 = turns(small[:, None] * small[None, :], 8)
    eye = np.eye(8)
    cos, sin = np.kron(eye, cos8), np.kron(eye, sin8)
    out["eight_fwd"] = halves(np.block([[cos, sin], [-sin, cos]]))
    out["eight_inv"] = halves(np.block([[cos, -sin], [sin, cos]]))
    row = np.arange(64)
    tile = row % 8 * 8 + row // 8
    place = np.argsort(tile)
    flips = []
    for source in (63 - tile, (64 - tile) % 64):
        one = np.zeros((64, 64))
        one[row, place[source]] = 1.0
        flips.append(np.kron(np.diag([1.0, -1.0]), one))
    out["flip_tile"] = np.concatenate(flips, axis=0).astype(ml_dtypes.bfloat16)
    cell = np.arange(CELLS)
    target = (8 - cell // 32) % 8 * 32 + (32 - cell % 32) % 32
    flip = np.zeros((CELLS, CELLS))
    flip[target, cell] = 1.0
    out["flip_cell"] = flip.astype(ml_dtypes.bfloat16)
    share = np.zeros((DEV, 8))
    share[: DEV // 2, :4] = 2.0
    share[DEV // 2 :, 1:5] = 2.0
    share[0, 0] = 1.0
    share[DEV // 2, 0] = 1.0
    share = np.repeat(share, ROWS, axis=1)
    out["share"] = np.concatenate([share, share], axis=1).astype(np.float32)
    return out


def split(x):
    high = x.astype(BF16)
    return high, (x - high.astype(F32)).astype(BF16)


def dot(a, b, dims=((1,), (0,))):
    return lax.dot_general(a, b, (dims, ((), ())), preferred_element_type=F32)


def dot3(a, b, dims=((1,), (0,))):
    (ah, al), (bh, bl) = a, b
    rows = ah.shape[0]
    both = dot(jnp.concatenate([ah, al], axis=0), bh, dims)
    return both[:rows] + (both[rows:] + dot(ah, bl, dims))


NT = ((1,), (1,))


def load_pair(high_ref, low_ref):
    return high_ref[...], low_ref[...]


def swap_chunks(x):
    chunk = lax.broadcasted_iota(jnp.int32, (8, LANES), 1) // 32
    blocks = {}
    for part in range(2):
        for a_high in range(2):
            for b_high in range(2):
                source = [
                    x[
                        part * 64 + (a_high * 4 + a) * 8 : part * 64 + (a_high * 4 + a) * 8 + 8,
                        b_high * LANES : (b_high + 1) * LANES,
                    ]
                    for a in range(4)
                ]
                for b in range(4):
                    made = None
                    for a in range(4):
                        shift = (a - b) * 32 % LANES
                        moved = source[a] if shift == 0 else pltpu.roll(source[a], shift, 1)
                        made = moved if made is None else jnp.where(chunk == a, moved, made)
                    blocks[part, b_high * 4 + b, a_high] = made
    rows = [
        jnp.concatenate([blocks[part, b, 0], blocks[part, b, 1]], axis=1)
        for part in range(2)
        for b in range(8)
    ]
    return jnp.concatenate(rows, axis=0)


def fold(x):
    squares = x * x
    total = None
    for i in range(x.shape[0] // 8):
        for j in range(x.shape[1] // LANES):
            piece = squares[i * 8 : i * 8 + 8, j * LANES : (j + 1) * LANES]
            total = piece if total is None else total + piece
    return total


def apply_matrix(spectrum, samples, mask_ref):
    parts = split(spectrum)
    row = lax.broadcasted_iota(jnp.int32, (LANES, 256), 0)
    tile = (row % 8 * 8 + row // 8 % 8).astype(F32)
    total = None
    for m in range(SAMPLES // 256):
        a = samples(m)
        seen = dot3(parts, a, NT)
        weight = mask_ref[m : m + 1, :]
        wanted = mask_ref[8 + m : 9 + m, :]
        kept = jnp.where(tile == wanted, seen * weight, 0.0)
        added = dot3(split(kept), a)
        total = added if total is None else total + added
    return total


def stored_samples(ah_ref, al_ref):
    return lambda m: (ah_ref[pl.ds(m * 256, 256), :], al_ref[pl.ds(m * 256, 256), :])


def pack_edge(grid):
    chunk = lax.broadcasted_iota(jnp.int32, (32, LANES), 1) // 32
    made = grid[:32, :LANES]
    for i in range(1, 4):
        moved = pltpu.roll(grid[i * 32 : i * 32 + 32, :LANES], i * 32, 1)
        made = jnp.where(chunk == i, moved, made)
    return made


def unpack_edge(edge):
    return jnp.concatenate(
        [edge] + [pltpu.roll(edge, LANES - i * 32, 1) for i in range(1, 4)], axis=0
    )


def mirrored(own_ref, other_ref, sent_ref, edge_ref, alone_ref, flip_tile_ref, flip_cell_ref):
    lane = lax.broadcasted_iota(jnp.int32, (LANES, CELLS), 1)
    other = other_ref[...]
    edge = jnp.where(alone_ref[0, 0] > 0, sent_ref[...], edge_ref[...])
    edge = jnp.concatenate([unpack_edge(edge), other[:, LANES:]], axis=1)
    other = jnp.where(lane < 32, edge, other)
    high, low = split(other)
    flips = flip_tile_ref[...]
    turned = dot(jnp.concatenate([flips, flips], axis=1), jnp.concatenate([high, low], axis=0))
    turned = jnp.where(lane % 32 == 0, turned[LANES:], turned[:LANES])
    high, low = split(turned)
    flip = flip_cell_ref[...]
    turned = dot(jnp.concatenate([high, low], axis=0), flip)
    return 0.5 * (own_ref[...] + (turned[:LANES] + turned[LANES:]))


def pack_kernel(image_hbm, interp_hbm, weight_hbm, index_hbm, counts_hbm, turn_hbm,
                out_hbm, out_ref, image_ref, held, weight_ref, index_ref, counts_ref,
                turn_ref, table_ref, sems):
    pieces = 8
    size = SLOTS // pieces
    pairs = [
        (turn_hbm, turn_ref), (image_hbm, image_ref),
        (index_hbm, index_ref), (counts_hbm, counts_ref), (weight_hbm, weight_ref),
    ]
    pairs += [
        (interp_hbm.at[pl.ds(i * size, size)], held.at[pl.ds(i * size, size)])
        for i in range(pieces)
    ]
    copies = [
        pltpu.make_async_copy(source, target, sems.at[i])
        for i, (source, target) in enumerate(pairs)
    ]
    for copy in copies:
        copy.start()
    copies[0].wait()
    cos_b, sin_b = turn_ref[16:32, :], turn_ref[32:48, :]
    for a in range(16):
        cos_a, sin_a = turn_ref[48 + a : 49 + a, :], turn_ref[64 + a : 65 + a, :]
        rows = slice(a * 16, a * 16 + 16)
        table_ref[0, rows, :DEV], table_ref[1, rows, :DEV] = split(cos_a * cos_b - sin_a * sin_b)
        table_ref[0, rows, DEV:], table_ref[1, rows, DEV:] = split(sin_a * cos_b + cos_a * sin_b)
    copies[1].wait()
    image = image_ref[...]
    x = [image[:, q * 256 : (q + 1) * 256] for q in range(8)]
    re, im = [None] * 8, [None] * 8
    for c in range(5):
        cos = [math.cos(2.0 * math.pi * (c * q % 8) / 8) for q in range(8)]
        sin = [math.sin(2.0 * math.pi * (c * q % 8) / 8) for q in range(8)]
        re[c] = sum(x[q] * cos[q] for q in range(1, 8)) + x[0]
        im[c] = jnp.zeros_like(x[0]) if c % 4 == 0 else -sum(x[q] * sin[q] for q in range(1, 8))
        if 0 < c < 4:
            re[8 - c] = re[c]
            im[8 - c] = -im[c]
    turned_re, turned_im = [], []
    for c in range(8):
        cos, sin = turn_ref[c : c + 1, :], turn_ref[8 + c : 9 + c, :]
        turned_re.append(re[c] * cos + im[c] * sin)
        turned_im.append(im[c] * cos - re[c] * sin)
    plain = jnp.concatenate(turned_re + turned_im, axis=0)
    crossed = jnp.concatenate(turned_im + [-v for v in turned_re], axis=0)
    data = split(jnp.concatenate([plain, crossed], axis=1))
    columns = dot3((table_ref[0], table_ref[1]), data, NT)
    for i in (2, 3, 4):
        copies[i].wait()
    marks = jnp.concatenate(
        [
            jnp.zeros((MARK_LANE, SLOTS), F32),
            weight_ref[...],
            index_ref[...].astype(F32),
            counts_ref[...].astype(F32),
            jnp.zeros((LANES - MARK_LANE - 10, SLOTS), F32),
        ],
        axis=0,
    )
    lane = lax.broadcasted_iota(jnp.int32, (DEV, LANES), 1)
    here = (lane >= MARK_LANE) & (lane < 64)
    out_ref[pl.ds(16, DEV, stride=MSG), :] = jnp.where(here, marks.T, columns)

    def move(group, carry):
        base = pl.multiple_of(group * (GROUP * MSG), 8)
        for m in range(GROUP):
            for tile in range(2):
                out_ref[pl.ds(base + m * MSG + tile * 8, 8), :] = held[
                    group * GROUP + m, :, tile * LANES : (tile + 1) * LANES
                ]
        return carry

    groups = SLOTS // GROUP // pieces
    rows = size * MSG
    sent = []
    for i in range(pieces):
        copies[5 + i].wait()
        lax.fori_loop(i * groups, (i + 1) * groups, move, 0, unroll=2)
        part = pl.ds(i * rows, rows)
        sent.append(
            pltpu.make_async_copy(out_ref.at[part], out_hbm.at[part], sems.at[13 + i])
        )
        sent[-1].start()
    for copy in sent:
        copy.wait()


def row_kernel(got_ref, row_ref):
    row_ref[...] = got_ref[pl.ds(16, DEV, stride=MSG), :]


def unpack_kernel(got_ref, row_ref, ah_ref, al_ref, mask_ref, turned_ref):
    for pair in range(SLOTS // 2):
        rows = [
            jnp.concatenate(
                [got_ref[pl.ds(slot * MSG + t * 8, 8), :] for t in range(2)], axis=1
            )
            for slot in (2 * pair, 2 * pair + 1)
        ]
        high, low = split(jnp.concatenate(rows, axis=0))
        ah_ref[pl.ds(pair * 16, 16), :] = high
        al_ref[pl.ds(pair * 16, 16), :] = low

    turned = row_ref[...].T
    turned_ref[...] = turned
    marks = turned[MARK_LANE : MARK_LANE + 16]
    chunk = lax.broadcasted_iota(jnp.int32, (16, SLOTS), 1) // 32
    stacked = jnp.concatenate([jnp.where(chunk == m, marks, 0.0) for m in range(8)], axis=0)
    high, low = split(stacked)
    lowest = (stacked - high.astype(F32) - low.astype(F32)).astype(BF16)
    slot = lax.broadcasted_iota(jnp.int32, (SLOTS, 256), 0) % 32
    spread = slot == lax.broadcasted_iota(jnp.int32, (SLOTS, 256), 1) // VCAP
    spread = jnp.where(spread, 1.0, 0.0).astype(BF16)
    spread_marks = dot(high, spread) + (dot(low, spread) + dot(lowest, spread))
    sample = lax.broadcasted_iota(jnp.int32, (8, 256), 1) % 8
    row = lax.broadcasted_iota(jnp.int32, (8, 256), 0)
    for m in range(8):
        block = spread_marks[m * 16 : m * 16 + 16]
        weight = jnp.sum(jnp.where(sample == row, block[:8], 0.0), axis=0, keepdims=True)
        live = sample[:1].astype(F32) < block[9:10]
        mask_ref[m : m + 1, :] = jnp.where(live, weight, 0.0)
        mask_ref[8 + m : 9 + m, :] = block[8:9]


def first_kernel(turned_ref, other_ref, ah_ref, al_ref, mask_ref, th_ref, tl_ref, turn_ref,
                 eh_ref, el_ref, out_ref, edge_ref, norm_ref):
    own, other = turned_ref[...], other_ref[...].T
    columns = jnp.concatenate(
        [own[:40]] + [other[c * 8 : c * 8 + 8] for c in (3, 2, 1)]
        + [own[64:104]] + [-other[64 + c * 8 : 72 + c * 8] for c in (3, 2, 1)],
        axis=0,
    )
    both = dot3(split(columns), load_pair(th_ref, tl_ref))
    by_cos, by_sin = both[:, :DEV], both[:, DEV:]
    re = (by_cos[:64] + by_sin[64:]).reshape(8, 8, DEV)
    im = (by_cos[64:] - by_sin[:64]).reshape(8, 8, DEV)
    scale = START_SCALE / N
    cos, sin = turn_ref[:8, :] * scale, turn_ref[8:, :] * scale
    turned = jnp.concatenate([re * cos + im * sin, im * cos - re * sin], axis=0)
    spectrum = dot3(load_pair(eh_ref, el_ref), split(turned.reshape(LANES, DEV)))
    spectrum = swap_chunks(spectrum)
    norm_ref[...] = fold(spectrum)
    grid = apply_matrix(spectrum, stored_samples(ah_ref, al_ref), mask_ref)
    out_ref[...] = grid
    edge_ref[...] = pack_edge(grid)


def next_kernel(own_ref, other_ref, sent_ref, edge_ref, alone_ref, ah_ref, al_ref, mask_ref, ft_ref, fc_ref,
                out_ref, edge_out_ref, norm_ref):
    spectrum = mirrored(own_ref, other_ref, sent_ref, edge_ref, alone_ref, ft_ref, fc_ref)
    norm_ref[...] = fold(spectrum)
    grid = apply_matrix(spectrum, stored_samples(ah_ref, al_ref), mask_ref)
    out_ref[...] = grid
    edge_out_ref[...] = pack_edge(grid)


def send_kernel(own_ref, other_ref, sent_ref, edge_ref, alone_ref, n0_ref, n1_ref, n2_ref, ft_ref, fc_ref,
                th_ref, tl_ref, turn_ref, eh_ref, el_ref, out_ref):
    spectrum = mirrored(own_ref, other_ref, sent_ref, edge_ref, alone_ref, ft_ref, fc_ref)
    norms = [jnp.sum(n) for n in (n0_ref[...], n1_ref[...], n2_ref[...], fold(spectrum))]
    data = dot3(load_pair(eh_ref, el_ref), split(swap_chunks(spectrum)))
    re = data[:64].reshape(8, 8, DEV)
    im = data[64:].reshape(8, 8, DEV)
    cos, sin = turn_ref[:8, :] * (1.0 / N), turn_ref[8:, :] * (1.0 / N)
    turned_re = (re * cos - im * sin).reshape(64, DEV)
    turned_im = (im * cos + re * sin).reshape(64, DEV)
    plain = jnp.concatenate([turned_re, turned_im], axis=0)
    crossed = jnp.concatenate([-turned_im, turned_re], axis=0)
    data = split(jnp.concatenate([plain, crossed], axis=1))
    out = dot3(load_pair(th_ref, tl_ref), data, NT)
    lane = lax.broadcasted_iota(jnp.int32, (DEV, LANES), 1)
    for i in range(4):
        out = jnp.where(lane == NORM_LANE + i, norms[i], out)
    out_ref[...] = out


def last_kernel(got_ref, share_ref, th_ref, tl_ref, turn_ref, image_ref, found_ref):
    got = got_ref[...]
    totals = jnp.sum(got, axis=0, keepdims=True)
    norms = [jnp.sqrt(totals[:, NORM_LANE + i : NORM_LANE + i + 1]) for i in range(4)]
    first = norms[1] / norms[0]
    rest = [norms[2] / norms[1], norms[3] / norms[2]]
    lane = lax.broadcasted_iota(jnp.int32, (1, 3), 1)
    found_ref[...] = jnp.where(lane == 0, first, jnp.where(lane == 1, rest[0], rest[1]))
    both = dot3(split((got * share_ref[...]).T), load_pair(th_ref, tl_ref))
    by_cos, by_sin = both[:, :DEV], both[:, DEV:]
    factor = float(N) / norms[3]
    re, im = [], []
    for c in range(5):
        here, there = slice(c * 8, c * 8 + 8), slice(64 + c * 8, 72 + c * 8)
        r = by_cos[here] - by_sin[there]
        i = by_cos[there] + by_sin[here]
        cos, sin = turn_ref[c : c + 1, :] * factor, turn_ref[8 + c : 9 + c, :] * factor
        re.append(r * cos - i * sin)
        im.append(i * cos + r * sin)
    for j in range(8):
        total = re[0]
        for c in range(1, 5):
            cos = math.cos(2.0 * math.pi * (c * j % 8) / 8)
            sin = math.sin(2.0 * math.pi * (c * j % 8) / 8)
            total = total + re[c] * cos - im[c] * sin
        image_ref[:, j * 256 : (j + 1) * 256] = total


def call(kernel, outs, in_specs, flops, moved, scratch=(), limit=24 * 2**20, out_specs=None):
    return pl.pallas_call(
        kernel,
        out_shape=tuple(jax.ShapeDtypeStruct(s, t) for s, t in outs),
        in_specs=in_specs,
        out_specs=out_specs or tuple(VMEM for _ in outs),
        scratch_shapes=list(scratch),
        compiler_params=pltpu.CompilerParams(vmem_limit_bytes=limit),
        cost_estimate=pl.CostEstimate(flops=flops, bytes_accessed=moved, transcendentals=0),
    )


def exchange(message):
    rows = message.shape[0]
    out = lax.all_to_all(
        message.reshape(rows, 1, LANES), AXES, 0, 0, tiled=True, axis_index_groups=[PLACES]
    )
    return out.reshape(rows, LANES)


def mirror_exchange(grid, edge, alone):
    got = lax.ppermute(edge, AXES, MIRROR_EDGE)
    other = lax.ppermute(grid, AXES, MIRROR)
    return grid, other, edge, got, alone


def per_device(image0, interp, vis_weight, counts, tile_index):
    t = {
        k: tuple(jnp.asarray(a) for a in v) if isinstance(v, tuple) else jnp.asarray(v)
        for k, v in tables().items()
    }
    pack = call(
        pack_kernel,
        [((DEV * MSG, LANES), F32)],
        [HBM] * 6,
        200_000_000,
        5_000_000,
        scratch=[
            pltpu.VMEM((DEV * MSG, LANES), F32),
            pltpu.VMEM((ROWS, N), F32),
            pltpu.VMEM((SLOTS, VCAP, CELLS), F32),
            pltpu.VMEM((VCAP, SLOTS), F32),
            pltpu.VMEM((1, SLOTS), jnp.int32),
            pltpu.VMEM((1, SLOTS), jnp.int32),
            pltpu.VMEM((80, DEV), F32),
            pltpu.VMEM((2, DEV, 2 * DEV), BF16),
            pltpu.SemaphoreType.DMA((21,)),
        ],
        limit=PACK_LIMIT,
        out_specs=(HBM,),
    )
    (message,) = pack(
        image0,
        interp.reshape(SLOTS, VCAP, CELLS),
        vis_weight.reshape(SLOTS, VCAP).T,
        tile_index.reshape(1, SLOTS),
        counts.reshape(1, SLOTS),
        t["start"],
    )
    got = exchange(message)
    (row,) = call(row_kernel, [((DEV, LANES), F32)], [VMEM], 100_000, 300_000)(got)
    other = lax.ppermute(row, AXES, MIRROR)
    a_high, a_low, mask, turned = call(
        unpack_kernel,
        [((SAMPLES, CELLS), BF16), ((SAMPLES, CELLS), BF16), ((16, 256), F32), ((LANES, DEV), F32)],
        [VMEM] * 2,
        100_000_000,
        5_000_000,
    )(got, row)
    first = call(
        first_kernel,
        [((LANES, CELLS), F32), ((32, LANES), F32), ((8, LANES), F32)],
        [VMEM] * 10,
        1_000_000_000,
        3_000_000,
    )
    grid, edge, n0 = first(
        turned, other, a_high, a_low, mask, *t["placed"], t["turn"], *t["eight_fwd"]
    )
    place = lax.axis_index(AXES)
    alone = (place == PLACES[SELF_EDGE[0]]) | (place == PLACES[SELF_EDGE[1]])
    alone = alone.astype(jnp.int32).reshape(1, 1)
    norms = [n0]
    follow = call(
        next_kernel,
        [((LANES, CELLS), F32), ((32, LANES), F32), ((8, LANES), F32)],
        [VMEM] * 4 + [SMEM] + [VMEM] * 5,
        1_000_000_000,
        3_000_000,
    )
    for _ in range(2):
        blocks = mirror_exchange(grid, edge, alone)
        grid, edge, norm = follow(
            *blocks, a_high, a_low, mask, t["flip_tile"], t["flip_cell"]
        )
        norms.append(norm)
    blocks = mirror_exchange(grid, edge, alone)
    send = call(
        send_kernel, [((DEV, LANES), F32)], [VMEM] * 4 + [SMEM] + [VMEM] * 10, 300_000_000, 1_500_000
    )
    (message,) = send(
        *blocks, *norms, t["flip_tile"], t["flip_cell"],
        *t["placed"], t["turn"], *t["eight_inv"],
    )
    got = exchange(message)
    last = call(
        last_kernel,
        [((ROWS, N), F32), ((1, 3), F32)],
        [VMEM] * 5,
        200_000_000,
        1_500_000,
    )
    image, found = last(got, t["share"], *t["plain"], t["turn"])
    return image, found.reshape(3)


def solution(mesh):
    in_specs = (
        P(AXES, None),
        P("base", "chan", None, None, None),
        P("base", "chan", None, None),
        P("base", "chan", None),
        P("base", "chan", None),
    )
    return jax.shard_map(
        per_device, mesh=mesh, in_specs=in_specs, out_specs=(P(AXES, None), P()), check_vma=False
    )
```

```python
import functools
import math

import jax
import jax.numpy as jnp
import ml_dtypes
import numpy as np
from jax import lax
from jax.experimental import pallas as pl
from jax.experimental.pallas import tpu as pltpu
from jax.sharding import PartitionSpec as P

AXES = ("base", "chan")
N = 2048
DEV = 256
ROWS = 8
CELLS = 256
SLOTS = 256
VCAP = 8
SAMPLES = SLOTS * VCAP
LANES = 128
MSG = 17
MARK_LANE = 40
GROUP = 8
START_SCALE = 2.0**-11
NORM_LANE = 40
PACK_LIMIT = 64_200_000
F32 = jnp.float32
BF16 = jnp.bfloat16
SMEM = pl.BlockSpec(memory_space=pltpu.SMEM)
VMEM = pl.BlockSpec(memory_space=pltpu.VMEM)
HBM = pl.BlockSpec(memory_space=pltpu.HBM)


def chip_path():
    path = []
    for z in range(8):
        plane = []
        for y in range(4):
            xs = range(4) if y % 2 == 0 else range(3, -1, -1)
            plane.extend((x, y, z) for x in xs)
        path.extend(plane if z % 2 == 0 else plane[::-1])
    return path


def block_places():
    places = [0] * DEV
    for o, (x, y, z) in enumerate(chip_path()):
        for core in range(2):
            place = (x * 8 + z % 4 * 2 + core) * 8 + y * 2 + z // 4
            places[o if core == 0 else DEV - 1 - o] = place
    return places


PLACES = block_places()
MIRROR = [(PLACES[o], PLACES[DEV - 1 - o]) for o in range(DEV)]
SELF_EDGE = (0, DEV // 2)
MIRROR_EDGE = [
    (PLACES[o], PLACES[DEV // 2 - o if o in SELF_EDGE else DEV - o]) for o in range(DEV)
]


def halves(table):
    high = table.astype(ml_dtypes.bfloat16)
    low = (table - high.astype(np.float64)).astype(ml_dtypes.bfloat16)
    return high, low


def turns(products, modulus):
    angle = 2.0 * np.pi * (np.asarray(products) % modulus) / modulus
    return np.cos(angle), np.sin(angle)


@functools.cache
def tables():
    out = {}
    index = np.arange(DEV)
    for name, rows in (("plain", index), ("placed", np.array(PLACES))):
        cos, sin = turns(rows[:, None] * index[None, :], DEV)
        out[name] = halves(np.concatenate([cos, sin], axis=1))
    few = np.arange(16)
    coarse = turns(few[:, None] * index[None, :], 16)
    fine = turns(few[:, None] * index[None, :], DEV)
    small = np.arange(8)
    cos, sin = turns(small[:, None] * index[None, :], N)
    out["turn"] = np.concatenate([cos, sin], axis=0).astype(np.float32)
    out["start"] = np.concatenate([cos, sin, *fine, *coarse], axis=0).astype(np.float32)
    cos8, sin8 = turns(small[:, None] * small[None, :], 8)
    eye = np.eye(8)
    cos, sin = np.kron(eye, cos8), np.kron(eye, sin8)
    out["eight_fwd"] = halves(np.block([[cos, sin], [-sin, cos]]))
    out["eight_inv"] = halves(np.block([[cos, -sin], [sin, cos]]))
    row = np.arange(64)
    tile = row % 8 * 8 + row // 8
    place = np.argsort(tile)
    flips = []
    for source in (63 - tile, (64 - tile) % 64):
        one = np.zeros((64, 64))
        one[row, place[source]] = 1.0
        flips.append(np.kron(np.diag([1.0, -1.0]), one))
    out["flip_tile"] = np.concatenate(flips, axis=0).astype(ml_dtypes.bfloat16)
    cell = np.arange(CELLS)
    target = (8 - cell // 32) % 8 * 32 + (32 - cell % 32) % 32
    flip = np.zeros((CELLS, CELLS))
    flip[target, cell] = 1.0
    out["flip_cell"] = flip.astype(ml_dtypes.bfloat16)
    share = np.zeros((DEV, 8))
    share[: DEV // 2, :4] = 2.0
    share[DEV // 2 :, 1:5] = 2.0
    share[0, 0] = 1.0
    share[DEV // 2, 0] = 1.0
    share = np.repeat(share, ROWS, axis=1)
    out["share"] = np.concatenate([share, share], axis=1).astype(np.float32)
    return out


def split(x):
    high = x.astype(BF16)
    return high, (x - high.astype(F32)).astype(BF16)


def dot(a, b, dims=((1,), (0,))):
    return lax.dot_general(a, b, (dims, ((), ())), preferred_element_type=F32)


def dot3(a, b, dims=((1,), (0,))):
    (ah, al), (bh, bl) = a, b
    rows = ah.shape[0]
    both = dot(jnp.concatenate([ah, al], axis=0), bh, dims)
    return both[:rows] + (both[rows:] + dot(ah, bl, dims))


NT = ((1,), (1,))


def load_pair(high_ref, low_ref):
    return high_ref[...], low_ref[...]


def swap_chunks(x):
    chunk = lax.broadcasted_iota(jnp.int32, (8, LANES), 1) // 32
    blocks = {}
    for part in range(2):
        for a_high in range(2):
            for b_high in range(2):
                source = [
                    x[
                        part * 64 + (a_high * 4 + a) * 8 : part * 64 + (a_high * 4 + a) * 8 + 8,
                        b_high * LANES : (b_high + 1) * LANES,
                    ]
                    for a in range(4)
                ]
                for b in range(4):
                    made = None
                    for a in range(4):
                        shift = (a - b) * 32 % LANES
                        moved = source[a] if shift == 0 else pltpu.roll(source[a], shift, 1)
                        made = moved if made is None else jnp.where(chunk == a, moved, made)
                    blocks[part, b_high * 4 + b, a_high] = made
    rows = [
        jnp.concatenate([blocks[part, b, 0], blocks[part, b, 1]], axis=1)
        for part in range(2)
        for b in range(8)
    ]
    return jnp.concatenate(rows, axis=0)


def fold(x):
    squares = x * x
    total = None
    for i in range(x.shape[0] // 8):
        for j in range(x.shape[1] // LANES):
            piece = squares[i * 8 : i * 8 + 8, j * LANES : (j + 1) * LANES]
            total = piece if total is None else total + piece
    return total


def apply_matrix(spectrum, samples, turned_samples, mask_ref):
    parts = split(spectrum)
    row = lax.broadcasted_iota(jnp.int32, (LANES, 256), 0)
    tile = (row % 8 * 8 + row // 8 % 8).astype(F32)
    total = None
    for m in range(SAMPLES // 256):
        a = samples(m)
        seen = dot3(parts, turned_samples(m))
        weight = mask_ref[m : m + 1, :]
        wanted = mask_ref[8 + m : 9 + m, :]
        kept = jnp.where(tile == wanted, seen * weight, 0.0)
        added = dot3(split(kept), a)
        total = added if total is None else total + added
    return total


def stored_samples(ah_ref, al_ref):
    return lambda m: (ah_ref[pl.ds(m * 256, 256), :], al_ref[pl.ds(m * 256, 256), :])


def stored_turned(ah_ref, al_ref):
    return lambda m: (ah_ref[:, pl.ds(m * 256, 256)], al_ref[:, pl.ds(m * 256, 256)])


def pack_edge(grid):
    chunk = lax.broadcasted_iota(jnp.int32, (32, LANES), 1) // 32
    made = grid[:32, :LANES]
    for i in range(1, 4):
        moved = pltpu.roll(grid[i * 32 : i * 32 + 32, :LANES], i * 32, 1)
        made = jnp.where(chunk == i, moved, made)
    return made


def unpack_edge(edge):
    return jnp.concatenate(
        [edge] + [pltpu.roll(edge, LANES - i * 32, 1) for i in range(1, 4)], axis=0
    )


def mirrored(own_ref, other_ref, sent_ref, edge_ref, alone_ref, flip_tile_ref, flip_cell_ref):
    lane = lax.broadcasted_iota(jnp.int32, (LANES, CELLS), 1)
    other = other_ref[...]
    edge = jnp.where(alone_ref[0, 0] > 0, sent_ref[...], edge_ref[...])
    edge = jnp.concatenate([unpack_edge(edge), other[:, LANES:]], axis=1)
    other = jnp.where(lane < 32, edge, other)
    high, low = split(other)
    flips = flip_tile_ref[...]
    turned = dot(jnp.concatenate([flips, flips], axis=1), jnp.concatenate([high, low], axis=0))
    turned = jnp.where(lane % 32 == 0, turned[LANES:], turned[:LANES])
    high, low = split(turned)
    flip = flip_cell_ref[...]
    turned = dot(jnp.concatenate([high, low], axis=0), flip)
    return 0.5 * (own_ref[...] + (turned[:LANES] + turned[LANES:]))


def pack_kernel(image_hbm, interp_hbm, weight_hbm, index_hbm, counts_hbm, turn_hbm,
                out_hbm, out_ref, image_ref, held, weight_ref, index_ref, counts_ref,
                turn_ref, table_ref, sems):
    pieces = 8
    size = SLOTS // pieces
    pairs = [
        (turn_hbm, turn_ref), (image_hbm, image_ref),
        (index_hbm, index_ref), (counts_hbm, counts_ref), (weight_hbm, weight_ref),
    ]
    pairs += [
        (interp_hbm.at[pl.ds(i * size, size)], held.at[pl.ds(i * size, size)])
        for i in range(pieces)
    ]
    copies = [
        pltpu.make_async_copy(source, target, sems.at[i])
        for i, (source, target) in enumerate(pairs)
    ]
    for copy in copies:
        copy.start()
    copies[0].wait()
    cos_b, sin_b = turn_ref[16:32, :], turn_ref[32:48, :]
    for a in range(16):
        cos_a, sin_a = turn_ref[48 + a : 49 + a, :], turn_ref[64 + a : 65 + a, :]
        rows = slice(a * 16, a * 16 + 16)
        table_ref[0, rows, :DEV], table_ref[1, rows, :DEV] = split(cos_a * cos_b - sin_a * sin_b)
        table_ref[0, rows, DEV:], table_ref[1, rows, DEV:] = split(sin_a * cos_b + cos_a * sin_b)
    copies[1].wait()
    image = image_ref[...]
    x = [image[:, q * 256 : (q + 1) * 256] for q in range(8)]
    re, im = [None] * 8, [None] * 8
    for c in range(5):
        cos = [math.cos(2.0 * math.pi * (c * q % 8) / 8) for q in range(8)]
        sin = [math.sin(2.0 * math.pi * (c * q % 8) / 8) for q in range(8)]
        re[c] = sum(x[q] * cos[q] for q in range(1, 8)) + x[0]
        im[c] = jnp.zeros_like(x[0]) if c % 4 == 0 else -sum(x[q] * sin[q] for q in range(1, 8))
        if 0 < c < 4:
            re[8 - c] = re[c]
            im[8 - c] = -im[c]
    turned_re, turned_im = [], []
    for c in range(8):
        cos, sin = turn_ref[c : c + 1, :], turn_ref[8 + c : 9 + c, :]
        turned_re.append(re[c] * cos + im[c] * sin)
        turned_im.append(im[c] * cos - re[c] * sin)
    plain = jnp.concatenate(turned_re + turned_im, axis=0)
    crossed = jnp.concatenate(turned_im + [-v for v in turned_re], axis=0)
    data = split(jnp.concatenate([plain, crossed], axis=1))
    columns = dot3((table_ref[0], table_ref[1]), data, NT)
    for i in (2, 3, 4):
        copies[i].wait()
    marks = jnp.concatenate(
        [
            jnp.zeros((MARK_LANE, SLOTS), F32),
            weight_ref[...],
            index_ref[...].astype(F32),
            counts_ref[...].astype(F32),
            jnp.zeros((LANES - MARK_LANE - 10, SLOTS), F32),
        ],
        axis=0,
    )
    lane = lax.broadcasted_iota(jnp.int32, (DEV, LANES), 1)
    here = (lane >= MARK_LANE) & (lane < 64)
    out_ref[pl.ds(16, DEV, stride=MSG), :] = jnp.where(here, marks.T, columns)

    def move(group, carry):
        base = pl.multiple_of(group * (GROUP * MSG), 8)
        for m in range(GROUP):
            for tile in range(2):
                out_ref[pl.ds(base + m * MSG + tile * 8, 8), :] = held[
                    group * GROUP + m, :, tile * LANES : (tile + 1) * LANES
                ]
        return carry

    groups = SLOTS // GROUP // pieces
    rows = size * MSG
    sent = []
    for i in range(pieces):
        copies[5 + i].wait()
        lax.fori_loop(i * groups, (i + 1) * groups, move, 0, unroll=2)
        part = pl.ds(i * rows, rows)
        sent.append(
            pltpu.make_async_copy(out_ref.at[part], out_hbm.at[part], sems.at[13 + i])
        )
        sent[-1].start()
    for copy in sent:
        copy.wait()


def row_kernel(got_ref, row_ref):
    row_ref[...] = got_ref[pl.ds(16, DEV, stride=MSG), :]


def unpack_kernel(got_ref, row_ref, ah_ref, al_ref, bh_ref, bl_ref, mask_ref, turned_ref):
    for part in range(SLOTS // 16):
        tiles = [[], []]
        for slot in range(part * 16, part * 16 + 16):
            for t in range(2):
                tiles[t].append(got_ref[pl.ds(slot * MSG + t * 8, 8), :])
        for t in range(2):
            tile = jnp.concatenate(tiles[t], axis=0)
            here, there = pl.ds(part * LANES, LANES), pl.ds(t * LANES, LANES)
            ah_ref[here, there], al_ref[here, there] = split(tile)
            bh_ref[there, here], bl_ref[there, here] = split(tile.T)

    turned = row_ref[...].T
    turned_ref[...] = turned
    marks = turned[MARK_LANE : MARK_LANE + 16]
    chunk = lax.broadcasted_iota(jnp.int32, (16, SLOTS), 1) // 32
    stacked = jnp.concatenate([jnp.where(chunk == m, marks, 0.0) for m in range(8)], axis=0)
    high, low = split(stacked)
    lowest = (stacked - high.astype(F32) - low.astype(F32)).astype(BF16)
    slot = lax.broadcasted_iota(jnp.int32, (SLOTS, 256), 0) % 32
    spread = slot == lax.broadcasted_iota(jnp.int32, (SLOTS, 256), 1) // VCAP
    spread = jnp.where(spread, 1.0, 0.0).astype(BF16)
    spread_marks = dot(high, spread) + (dot(low, spread) + dot(lowest, spread))
    sample = lax.broadcasted_iota(jnp.int32, (8, 256), 1) % 8
    row = lax.broadcasted_iota(jnp.int32, (8, 256), 0)
    for m in range(8):
        block = spread_marks[m * 16 : m * 16 + 16]
        weight = jnp.sum(jnp.where(sample == row, block[:8], 0.0), axis=0, keepdims=True)
        live = sample[:1].astype(F32) < block[9:10]
        mask_ref[m : m + 1, :] = jnp.where(live, weight, 0.0)
        mask_ref[8 + m : 9 + m, :] = block[8:9]


def first_kernel(turned_ref, other_ref, ah_ref, al_ref, bh_ref, bl_ref, mask_ref, th_ref, tl_ref, turn_ref,
                 eh_ref, el_ref, out_ref, edge_ref, norm_ref):
    own, other = turned_ref[...], other_ref[...].T
    columns = jnp.concatenate(
        [own[:40]] + [other[c * 8 : c * 8 + 8] for c in (3, 2, 1)]
        + [own[64:104]] + [-other[64 + c * 8 : 72 + c * 8] for c in (3, 2, 1)],
        axis=0,
    )
    both = dot3(split(columns), load_pair(th_ref, tl_ref))
    by_cos, by_sin = both[:, :DEV], both[:, DEV:]
    re = (by_cos[:64] + by_sin[64:]).reshape(8, 8, DEV)
    im = (by_cos[64:] - by_sin[:64]).reshape(8, 8, DEV)
    scale = START_SCALE / N
    cos, sin = turn_ref[:8, :] * scale, turn_ref[8:, :] * scale
    turned = jnp.concatenate([re * cos + im * sin, im * cos - re * sin], axis=0)
    spectrum = dot3(load_pair(eh_ref, el_ref), split(turned.reshape(LANES, DEV)))
    spectrum = swap_chunks(spectrum)
    norm_ref[...] = fold(spectrum)
    grid = apply_matrix(
        spectrum, stored_samples(ah_ref, al_ref), stored_turned(bh_ref, bl_ref), mask_ref
    )
    out_ref[...] = grid
    edge_ref[...] = pack_edge(grid)


def next_kernel(own_ref, other_ref, sent_ref, edge_ref, alone_ref, ah_ref, al_ref, bh_ref, bl_ref, mask_ref, ft_ref, fc_ref,
                out_ref, edge_out_ref, norm_ref):
    spectrum = mirrored(own_ref, other_ref, sent_ref, edge_ref, alone_ref, ft_ref, fc_ref)
    norm_ref[...] = fold(spectrum)
    grid = apply_matrix(
        spectrum, stored_samples(ah_ref, al_ref), stored_turned(bh_ref, bl_ref), mask_ref
    )
    out_ref[...] = grid
    edge_out_ref[...] = pack_edge(grid)


def send_kernel(own_ref, other_ref, sent_ref, edge_ref, alone_ref, n0_ref, n1_ref, n2_ref, ft_ref, fc_ref,
                th_ref, tl_ref, turn_ref, eh_ref, el_ref, out_ref):
    spectrum = mirrored(own_ref, other_ref, sent_ref, edge_ref, alone_ref, ft_ref, fc_ref)
    norms = [jnp.sum(n) for n in (n0_ref[...], n1_ref[...], n2_ref[...], fold(spectrum))]
    data = dot3(load_pair(eh_ref, el_ref), split(swap_chunks(spectrum)))
    re = data[:64].reshape(8, 8, DEV)
    im = data[64:].reshape(8, 8, DEV)
    cos, sin = turn_ref[:8, :] * (1.0 / N), turn_ref[8:, :] * (1.0 / N)
    turned_re = (re * cos - im * sin).reshape(64, DEV)
    turned_im = (im * cos + re * sin).reshape(64, DEV)
    plain = jnp.concatenate([turned_re, turned_im], axis=0)
    crossed = jnp.concatenate([-turned_im, turned_re], axis=0)
    data = split(jnp.concatenate([plain, crossed], axis=1))
    out = dot3(load_pair(th_ref, tl_ref), data, NT)
    lane = lax.broadcasted_iota(jnp.int32, (DEV, LANES), 1)
    for i in range(4):
        out = jnp.where(lane == NORM_LANE + i, norms[i], out)
    out_ref[...] = out


def last_kernel(got_ref, share_ref, th_ref, tl_ref, turn_ref, image_ref, found_ref):
    got = got_ref[...]
    totals = jnp.sum(got, axis=0, keepdims=True)
    norms = [jnp.sqrt(totals[:, NORM_LANE + i : NORM_LANE + i + 1]) for i in range(4)]
    first = norms[1] / norms[0]
    rest = [norms[2] / norms[1], norms[3] / norms[2]]
    lane = lax.broadcasted_iota(jnp.int32, (1, 3), 1)
    found_ref[...] = jnp.where(lane == 0, first, jnp.where(lane == 1, rest[0], rest[1]))
    both = dot3(split((got * share_ref[...]).T), load_pair(th_ref, tl_ref))
    by_cos, by_sin = both[:, :DEV], both[:, DEV:]
    factor = float(N) / norms[3]
    re, im = [], []
    for c in range(5):
        here, there = slice(c * 8, c * 8 + 8), slice(64 + c * 8, 72 + c * 8)
        r = by_cos[here] - by_sin[there]
        i = by_cos[there] + by_sin[here]
        cos, sin = turn_ref[c : c + 1, :] * factor, turn_ref[8 + c : 9 + c, :] * factor
        re.append(r * cos - i * sin)
        im.append(i * cos + r * sin)
    for j in range(8):
        total = re[0]
        for c in range(1, 5):
            cos = math.cos(2.0 * math.pi * (c * j % 8) / 8)
            sin = math.sin(2.0 * math.pi * (c * j % 8) / 8)
            total = total + re[c] * cos - im[c] * sin
        image_ref[:, j * 256 : (j + 1) * 256] = total


def call(kernel, outs, in_specs, flops, moved, scratch=(), limit=24 * 2**20, out_specs=None):
    return pl.pallas_call(
        kernel,
        out_shape=tuple(jax.ShapeDtypeStruct(s, t) for s, t in outs),
        in_specs=in_specs,
        out_specs=out_specs or tuple(VMEM for _ in outs),
        scratch_shapes=list(scratch),
        compiler_params=pltpu.CompilerParams(vmem_limit_bytes=limit),
        cost_estimate=pl.CostEstimate(flops=flops, bytes_accessed=moved, transcendentals=0),
    )


def exchange(message):
    rows = message.shape[0]
    out = lax.all_to_all(
        message.reshape(rows, 1, LANES), AXES, 0, 0, tiled=True, axis_index_groups=[PLACES]
    )
    return out.reshape(rows, LANES)


def mirror_exchange(grid, edge, alone):
    got = lax.ppermute(edge, AXES, MIRROR_EDGE)
    other = lax.ppermute(grid, AXES, MIRROR)
    return grid, other, edge, got, alone


def per_device(image0, interp, vis_weight, counts, tile_index):
    t = {
        k: tuple(jnp.asarray(a) for a in v) if isinstance(v, tuple) else jnp.asarray(v)
        for k, v in tables().items()
    }
    pack = call(
        pack_kernel,
        [((DEV * MSG, LANES), F32)],
        [HBM] * 6,
        200_000_000,
        5_000_000,
        scratch=[
            pltpu.VMEM((DEV * MSG, LANES), F32),
            pltpu.VMEM((ROWS, N), F32),
            pltpu.VMEM((SLOTS, VCAP, CELLS), F32),
            pltpu.VMEM((VCAP, SLOTS), F32),
            pltpu.VMEM((1, SLOTS), jnp.int32),
            pltpu.VMEM((1, SLOTS), jnp.int32),
            pltpu.VMEM((80, DEV), F32),
            pltpu.VMEM((2, DEV, 2 * DEV), BF16),
            pltpu.SemaphoreType.DMA((21,)),
        ],
        limit=PACK_LIMIT,
        out_specs=(HBM,),
    )
    (message,) = pack(
        image0,
        interp.reshape(SLOTS, VCAP, CELLS),
        vis_weight.reshape(SLOTS, VCAP).T,
        tile_index.reshape(1, SLOTS),
        counts.reshape(1, SLOTS),
        t["start"],
    )
    got = exchange(message)
    (row,) = call(row_kernel, [((DEV, LANES), F32)], [VMEM], 100_000, 300_000)(got)
    other = lax.ppermute(row, AXES, MIRROR)
    *samples, mask, turned = call(
        unpack_kernel,
        [
            ((SAMPLES, CELLS), BF16),
            ((SAMPLES, CELLS), BF16),
            ((CELLS, SAMPLES), BF16),
            ((CELLS, SAMPLES), BF16),
            ((16, 256), F32),
            ((LANES, DEV), F32),
        ],
        [VMEM] * 2,
        100_000_000,
        5_000_000,
    )(got, row)
    first = call(
        first_kernel,
        [((LANES, CELLS), F32), ((32, LANES), F32), ((8, LANES), F32)],
        [VMEM] * 12,
        1_000_000_000,
        3_000_000,
    )
    grid, edge, n0 = first(
        turned, other, *samples, mask, *t["placed"], t["turn"], *t["eight_fwd"]
    )
    place = lax.axis_index(AXES)
    alone = (place == PLACES[SELF_EDGE[0]]) | (place == PLACES[SELF_EDGE[1]])
    alone = alone.astype(jnp.int32).reshape(1, 1)
    norms = [n0]
    follow = call(
        next_kernel,
        [((LANES, CELLS), F32), ((32, LANES), F32), ((8, LANES), F32)],
        [VMEM] * 4 + [SMEM] + [VMEM] * 7,
        1_000_000_000,
        3_000_000,
    )
    for _ in range(2):
        blocks = mirror_exchange(grid, edge, alone)
        grid, edge, norm = follow(
            *blocks, *samples, mask, t["flip_tile"], t["flip_cell"]
        )
        norms.append(norm)
    blocks = mirror_exchange(grid, edge, alone)
    send = call(
        send_kernel, [((DEV, LANES), F32)], [VMEM] * 4 + [SMEM] + [VMEM] * 10, 300_000_000, 1_500_000
    )
    (message,) = send(
        *blocks, *norms, t["flip_tile"], t["flip_cell"],
        *t["placed"], t["turn"], *t["eight_inv"],
    )
    got = exchange(message)
    last = call(
        last_kernel,
        [((ROWS, N), F32), ((1, 3), F32)],
        [VMEM] * 5,
        200_000_000,
        1_500_000,
    )
    image, found = last(got, t["share"], *t["plain"], t["turn"])
    return image, found.reshape(3)


def solution(mesh):
    in_specs = (
        P(AXES, None),
        P("base", "chan", None, None, None),
        P("base", "chan", None, None),
        P("base", "chan", None),
        P("base", "chan", None),
    )
    return jax.shard_map(
        per_device, mesh=mesh, in_specs=in_specs, out_specs=(P(AXES, None), P()), check_vma=False
    )
```

```python
import functools
import math

import jax
import jax.numpy as jnp
import ml_dtypes
import numpy as np
from jax import lax
from jax.experimental import pallas as pl
from jax.experimental.pallas import tpu as pltpu
from jax.sharding import PartitionSpec as P

AXES = ("base", "chan")
N = 2048
DEV = 256
ROWS = 8
CELLS = 256
SLOTS = 256
VCAP = 8
SAMPLES = SLOTS * VCAP
LANES = 128
MSG = 17
MARK_LANE = 40
GROUP = 8
START_SCALE = 2.0**-11
NORM_LANE = 40
PACK_LIMIT = 64_200_000
F32 = jnp.float32
BF16 = jnp.bfloat16
SMEM = pl.BlockSpec(memory_space=pltpu.SMEM)
VMEM = pl.BlockSpec(memory_space=pltpu.VMEM)
HBM = pl.BlockSpec(memory_space=pltpu.HBM)


def chip_path():
    path = []
    for z in range(8):
        plane = []
        for y in range(4):
            xs = range(4) if y % 2 == 0 else range(3, -1, -1)
            plane.extend((x, y, z) for x in xs)
        path.extend(plane if z % 2 == 0 else plane[::-1])
    return path


def block_places():
    places = [0] * DEV
    for o, (x, y, z) in enumerate(chip_path()):
        for core in range(2):
            place = (x * 8 + z % 4 * 2 + core) * 8 + y * 2 + z // 4
            places[o if core == 0 else DEV - 1 - o] = place
    return places


PLACES = block_places()
MIRROR = [(PLACES[o], PLACES[DEV - 1 - o]) for o in range(DEV)]
SELF_EDGE = (0, DEV // 2)
MIRROR_EDGE = [
    (PLACES[o], PLACES[DEV // 2 - o if o in SELF_EDGE else DEV - o]) for o in range(DEV)
]


def halves(table):
    high = table.astype(ml_dtypes.bfloat16)
    low = (table - high.astype(np.float64)).astype(ml_dtypes.bfloat16)
    return high, low


def turns(products, modulus):
    angle = 2.0 * np.pi * (np.asarray(products) % modulus) / modulus
    return np.cos(angle), np.sin(angle)


@functools.cache
def tables():
    out = {}
    index = np.arange(DEV)
    for name, rows in (("plain", index), ("placed", np.array(PLACES))):
        cos, sin = turns(rows[:, None] * index[None, :], DEV)
        out[name] = halves(np.concatenate([cos, sin], axis=1))
    few = np.arange(16)
    coarse = turns(few[:, None] * index[None, :], 16)
    fine = turns(few[:, None] * index[None, :], DEV)
    small = np.arange(8)
    cos, sin = turns(small[:, None] * index[None, :], N)
    out["turn"] = np.concatenate([cos, sin], axis=0).astype(np.float32)
    out["start"] = np.concatenate([cos, sin, *fine, *coarse], axis=0).astype(np.float32)
    cos8, sin8 = turns(small[:, None] * small[None, :], 8)
    eye = np.eye(8)
    cos, sin = np.kron(eye, cos8), np.kron(eye, sin8)
    out["eight_fwd"] = halves(np.block([[cos, sin], [-sin, cos]]))
    out["eight_inv"] = halves(np.block([[cos, -sin], [sin, cos]]))
    row = np.arange(64)
    tile = row % 8 * 8 + row // 8
    place = np.argsort(tile)
    flips = []
    for source in (63 - tile, (64 - tile) % 64):
        one = np.zeros((64, 64))
        one[row, place[source]] = 1.0
        flips.append(np.kron(np.diag([1.0, -1.0]), one))
    out["flip_tile"] = np.concatenate(flips, axis=0).astype(ml_dtypes.bfloat16)
    cell = np.arange(CELLS)
    target = (8 - cell // 32) % 8 * 32 + (32 - cell % 32) % 32
    flip = np.zeros((CELLS, CELLS))
    flip[target, cell] = 1.0
    out["flip_cell"] = flip.astype(ml_dtypes.bfloat16)
    share = np.zeros((DEV, 8))
    share[: DEV // 2, :4] = 2.0
    share[DEV // 2 :, 1:5] = 2.0
    share[0, 0] = 1.0
    share[DEV // 2, 0] = 1.0
    share = np.repeat(share, ROWS, axis=1)
    out["share"] = np.concatenate([share, share], axis=1).astype(np.float32)
    return out


def split(x):
    high = x.astype(BF16)
    return high, (x - high.astype(F32)).astype(BF16)


def dot(a, b, dims=((1,), (0,))):
    return lax.dot_general(a, b, (dims, ((), ())), preferred_element_type=F32)


def dot3(a, b, dims=((1,), (0,))):
    (ah, al), (bh, bl) = a, b
    rows = ah.shape[0]
    both = dot(jnp.concatenate([ah, al], axis=0), bh, dims)
    return both[:rows] + (both[rows:] + dot(ah, bl, dims))


NT = ((1,), (1,))


def load_pair(high_ref, low_ref):
    return high_ref[...], low_ref[...]


def swap_chunks(x):
    chunk = lax.broadcasted_iota(jnp.int32, (8, LANES), 1) // 32
    blocks = {}
    for part in range(2):
        for a_high in range(2):
            for b_high in range(2):
                source = [
                    x[
                        part * 64 + (a_high * 4 + a) * 8 : part * 64 + (a_high * 4 + a) * 8 + 8,
                        b_high * LANES : (b_high + 1) * LANES,
                    ]
                    for a in range(4)
                ]
                for b in range(4):
                    made = None
                    for a in range(4):
                        shift = (a - b) * 32 % LANES
                        moved = source[a] if shift == 0 else pltpu.roll(source[a], shift, 1)
                        made = moved if made is None else jnp.where(chunk == a, moved, made)
                    blocks[part, b_high * 4 + b, a_high] = made
    rows = [
        jnp.concatenate([blocks[part, b, 0], blocks[part, b, 1]], axis=1)
        for part in range(2)
        for b in range(8)
    ]
    return jnp.concatenate(rows, axis=0)


def fold(x):
    squares = x * x
    total = None
    for i in range(x.shape[0] // 8):
        for j in range(x.shape[1] // LANES):
            piece = squares[i * 8 : i * 8 + 8, j * LANES : (j + 1) * LANES]
            total = piece if total is None else total + piece
    return total


def apply_matrix(spectrum, samples, mask_ref):
    parts = split(spectrum)
    row = lax.broadcasted_iota(jnp.int32, (LANES, 256), 0)
    tile = (row % 8 * 8 + row // 8 % 8).astype(F32)
    total = None
    for m in range(SAMPLES // 256):
        a = samples(m)
        seen = dot3(parts, a, NT)
        weight = mask_ref[m : m + 1, :]
        wanted = mask_ref[8 + m : 9 + m, :]
        kept = jnp.where(tile == wanted, seen * weight, 0.0)
        added = dot3(split(kept), a)
        total = added if total is None else total + added
    return total


def stored_samples(ah_ref, al_ref):
    return lambda m: (ah_ref[pl.ds(m * 256, 256), :], al_ref[pl.ds(m * 256, 256), :])


def pack_edge(grid):
    chunk = lax.broadcasted_iota(jnp.int32, (32, LANES), 1) // 32
    made = grid[:32, :LANES]
    for i in range(1, 4):
        moved = pltpu.roll(grid[i * 32 : i * 32 + 32, :LANES], i * 32, 1)
        made = jnp.where(chunk == i, moved, made)
    return made


def unpack_edge(edge):
    return jnp.concatenate(
        [edge] + [pltpu.roll(edge, LANES - i * 32, 1) for i in range(1, 4)], axis=0
    )


def mirrored(own_ref, other_ref, sent_ref, edge_ref, alone_ref, flip_tile_ref, flip_cell_ref):
    lane = lax.broadcasted_iota(jnp.int32, (LANES, CELLS), 1)
    other = other_ref[...]
    edge = jnp.where(alone_ref[0, 0] > 0, sent_ref[...], edge_ref[...])
    edge = jnp.concatenate([unpack_edge(edge), other[:, LANES:]], axis=1)
    other = jnp.where(lane < 32, edge, other)
    high, low = split(other)
    flips = flip_tile_ref[...]
    turned = dot(jnp.concatenate([flips, flips], axis=1), jnp.concatenate([high, low], axis=0))
    turned = jnp.where(lane % 32 == 0, turned[LANES:], turned[:LANES])
    high, low = split(turned)
    flip = flip_cell_ref[...]
    turned = dot(jnp.concatenate([high, low], axis=0), flip)
    return 0.5 * (own_ref[...] + (turned[:LANES] + turned[LANES:]))


def pack_kernel(image_hbm, interp_hbm, weight_hbm, index_hbm, counts_hbm, turn_hbm,
                out_hbm, out_ref, image_ref, held, weight_ref, index_ref, counts_ref,
                turn_ref, table_ref, sems):
    pieces = 8
    size = SLOTS // pieces
    pairs = [
        (turn_hbm, turn_ref), (image_hbm, image_ref),
        (index_hbm, index_ref), (counts_hbm, counts_ref), (weight_hbm, weight_ref),
    ]
    pairs += [
        (interp_hbm.at[pl.ds(i * size, size)], held.at[pl.ds(i * size, size)])
        for i in range(pieces)
    ]
    copies = [
        pltpu.make_async_copy(source, target, sems.at[i])
        for i, (source, target) in enumerate(pairs)
    ]
    for copy in copies:
        copy.start()
    copies[0].wait()
    cos_b, sin_b = turn_ref[16:32, :], turn_ref[32:48, :]
    for a in range(16):
        cos_a, sin_a = turn_ref[48 + a : 49 + a, :], turn_ref[64 + a : 65 + a, :]
        rows = slice(a * 16, a * 16 + 16)
        table_ref[0, rows, :DEV], table_ref[1, rows, :DEV] = split(cos_a * cos_b - sin_a * sin_b)
        table_ref[0, rows, DEV:], table_ref[1, rows, DEV:] = split(sin_a * cos_b + cos_a * sin_b)
    copies[1].wait()
    image = image_ref[...]
    x = [image[:, q * 256 : (q + 1) * 256] for q in range(8)]
    re, im = [None] * 8, [None] * 8
    for c in range(5):
        cos = [math.cos(2.0 * math.pi * (c * q % 8) / 8) for q in range(8)]
        sin = [math.sin(2.0 * math.pi * (c * q % 8) / 8) for q in range(8)]
        re[c] = sum(x[q] * cos[q] for q in range(1, 8)) + x[0]
        im[c] = jnp.zeros_like(x[0]) if c % 4 == 0 else -sum(x[q] * sin[q] for q in range(1, 8))
        if 0 < c < 4:
            re[8 - c] = re[c]
            im[8 - c] = -im[c]
    turned_re, turned_im = [], []
    for c in range(8):
        cos, sin = turn_ref[c : c + 1, :], turn_ref[8 + c : 9 + c, :]
        turned_re.append(re[c] * cos + im[c] * sin)
        turned_im.append(im[c] * cos - re[c] * sin)
    plain = jnp.concatenate(turned_re + turned_im, axis=0)
    crossed = jnp.concatenate(turned_im + [-v for v in turned_re], axis=0)
    data = split(jnp.concatenate([plain, crossed], axis=1))
    columns = dot3((table_ref[0], table_ref[1]), data, NT)
    for i in (2, 3, 4):
        copies[i].wait()
    marks = jnp.concatenate(
        [
            jnp.zeros((MARK_LANE, SLOTS), F32),
            weight_ref[...],
            index_ref[...].astype(F32),
            counts_ref[...].astype(F32),
            jnp.zeros((LANES - MARK_LANE - 10, SLOTS), F32),
        ],
        axis=0,
    )
    lane = lax.broadcasted_iota(jnp.int32, (DEV, LANES), 1)
    here = (lane >= MARK_LANE) & (lane < 64)
    out_ref[pl.ds(16, DEV, stride=MSG), :] = jnp.where(here, marks.T, columns)

    def move(group, carry):
        base = pl.multiple_of(group * (GROUP * MSG), 8)
        for m in range(GROUP):
            for tile in range(2):
                out_ref[pl.ds(base + m * MSG + tile * 8, 8), :] = held[
                    group * GROUP + m, :, tile * LANES : (tile + 1) * LANES
                ]
        return carry

    groups = SLOTS // GROUP // pieces
    rows = size * MSG
    sent = []
    for i in range(pieces):
        copies[5 + i].wait()
        lax.fori_loop(i * groups, (i + 1) * groups, move, 0, unroll=2)
        part = pl.ds(i * rows, rows)
        sent.append(
            pltpu.make_async_copy(out_ref.at[part], out_hbm.at[part], sems.at[13 + i])
        )
        sent[-1].start()
    for copy in sent:
        copy.wait()


def row_kernel(got_ref, row_ref):
    row_ref[...] = got_ref[pl.ds(16, DEV, stride=MSG), :]


def unpack_kernel(got_ref, row_ref, ah_ref, al_ref, mask_ref, turned_ref):
    for pair in range(SLOTS // 2):
        rows = [
            jnp.concatenate(
                [got_ref[pl.ds(slot * MSG + t * 8, 8), :] for t in range(2)], axis=1
            )
            for slot in (2 * pair, 2 * pair + 1)
        ]
        high, low = split(jnp.concatenate(rows, axis=0))
        ah_ref[pl.ds(pair * 16, 16), :] = high
        al_ref[pl.ds(pair * 16, 16), :] = low

    turned = row_ref[...].T
    turned_ref[...] = turned
    marks = turned[MARK_LANE : MARK_LANE + 16]
    chunk = lax.broadcasted_iota(jnp.int32, (16, SLOTS), 1) // 32
    stacked = jnp.concatenate([jnp.where(chunk == m, marks, 0.0) for m in range(8)], axis=0)
    high, low = split(stacked)
    lowest = (stacked - high.astype(F32) - low.astype(F32)).astype(BF16)
    slot = lax.broadcasted_iota(jnp.int32, (SLOTS, 256), 0) % 32
    spread = slot == lax.broadcasted_iota(jnp.int32, (SLOTS, 256), 1) // VCAP
    spread = jnp.where(spread, 1.0, 0.0).astype(BF16)
    spread_marks = dot(high, spread) + (dot(low, spread) + dot(lowest, spread))
    sample = lax.broadcasted_iota(jnp.int32, (8, 256), 1) % 8
    row = lax.broadcasted_iota(jnp.int32, (8, 256), 0)
    for m in range(8):
        block = spread_marks[m * 16 : m * 16 + 16]
        weight = jnp.sum(jnp.where(sample == row, block[:8], 0.0), axis=0, keepdims=True)
        live = sample[:1].astype(F32) < block[9:10]
        mask_ref[m : m + 1, :] = jnp.where(live, weight, 0.0)
        mask_ref[8 + m : 9 + m, :] = block[8:9]


def first_kernel(turned_ref, other_ref, ah_ref, al_ref, mask_ref, th_ref, tl_ref, turn_ref,
                 eh_ref, el_ref, out_ref, edge_ref, norm_ref):
    own, other = turned_ref[...], other_ref[...].T
    columns = jnp.concatenate(
        [own[:40]] + [other[c * 8 : c * 8 + 8] for c in (3, 2, 1)]
        + [own[64:104]] + [-other[64 + c * 8 : 72 + c * 8] for c in (3, 2, 1)],
        axis=0,
    )
    both = dot3(split(columns), load_pair(th_ref, tl_ref))
    by_cos, by_sin = both[:, :DEV], both[:, DEV:]
    re = (by_cos[:64] + by_sin[64:]).reshape(8, 8, DEV)
    im = (by_cos[64:] - by_sin[:64]).reshape(8, 8, DEV)
    scale = START_SCALE / N
    cos, sin = turn_ref[:8, :] * scale, turn_ref[8:, :] * scale
    turned = jnp.concatenate([re * cos + im * sin, im * cos - re * sin], axis=0)
    spectrum = dot3(load_pair(eh_ref, el_ref), split(turned.reshape(LANES, DEV)))
    spectrum = swap_chunks(spectrum)
    norm_ref[...] = fold(spectrum)
    grid = apply_matrix(spectrum, stored_samples(ah_ref, al_ref), mask_ref)
    out_ref[...] = grid
    edge_ref[...] = pack_edge(grid)


def next_kernel(own_ref, other_ref, sent_ref, edge_ref, alone_ref, ah_ref, al_ref, mask_ref, ft_ref, fc_ref,
                out_ref, edge_out_ref, norm_ref):
    spectrum = mirrored(own_ref, other_ref, sent_ref, edge_ref, alone_ref, ft_ref, fc_ref)
    norm_ref[...] = fold(spectrum)
    grid = apply_matrix(spectrum, stored_samples(ah_ref, al_ref), mask_ref)
    out_ref[...] = grid
    edge_out_ref[...] = pack_edge(grid)


def send_kernel(own_ref, other_ref, sent_ref, edge_ref, alone_ref, n0_ref, n1_ref, n2_ref, ft_ref, fc_ref,
                th_ref, tl_ref, turn_ref, eh_ref, el_ref, out_ref):
    spectrum = mirrored(own_ref, other_ref, sent_ref, edge_ref, alone_ref, ft_ref, fc_ref)
    norms = [jnp.sum(n) for n in (n0_ref[...], n1_ref[...], n2_ref[...], fold(spectrum))]
    data = dot3(load_pair(eh_ref, el_ref), split(swap_chunks(spectrum)))
    re = data[:64].reshape(8, 8, DEV)
    im = data[64:].reshape(8, 8, DEV)
    cos, sin = turn_ref[:8, :] * (1.0 / N), turn_ref[8:, :] * (1.0 / N)
    turned_re = (re * cos - im * sin).reshape(64, DEV)
    turned_im = (im * cos + re * sin).reshape(64, DEV)
    plain = jnp.concatenate([turned_re, turned_im], axis=0)
    crossed = jnp.concatenate([-turned_im, turned_re], axis=0)
    data = split(jnp.concatenate([plain, crossed], axis=1))
    out = dot3(load_pair(th_ref, tl_ref), data, NT)
    lane = lax.broadcasted_iota(jnp.int32, (DEV, LANES), 1)
    for i in range(4):
        out = jnp.where(lane == NORM_LANE + i, norms[i], out)
    out_ref[...] = out


def last_kernel(got_ref, share_ref, th_ref, tl_ref, turn_ref, image_hbm, found_ref, image_ref, sems):
    got = got_ref[...]
    totals = jnp.sum(got, axis=0, keepdims=True)
    norms = [jnp.sqrt(totals[:, NORM_LANE + i : NORM_LANE + i + 1]) for i in range(4)]
    first = norms[1] / norms[0]
    rest = [norms[2] / norms[1], norms[3] / norms[2]]
    lane = lax.broadcasted_iota(jnp.int32, (1, 3), 1)
    found_ref[...] = jnp.where(lane == 0, first, jnp.where(lane == 1, rest[0], rest[1]))
    both = dot3(split((got * share_ref[...]).T), load_pair(th_ref, tl_ref))
    by_cos, by_sin = both[:, :DEV], both[:, DEV:]
    factor = float(N) / norms[3]
    re, im = [], []
    for c in range(5):
        here, there = slice(c * 8, c * 8 + 8), slice(64 + c * 8, 72 + c * 8)
        r = by_cos[here] - by_sin[there]
        i = by_cos[there] + by_sin[here]
        cos, sin = turn_ref[c : c + 1, :] * factor, turn_ref[8 + c : 9 + c, :] * factor
        re.append(r * cos - i * sin)
        im.append(i * cos + r * sin)
    sent = []
    for j in range(8):
        total = re[0]
        for c in range(1, 5):
            cos = math.cos(2.0 * math.pi * (c * j % 8) / 8)
            sin = math.sin(2.0 * math.pi * (c * j % 8) / 8)
            total = total + re[c] * cos - im[c] * sin
        image_ref[:, j * 256 : (j + 1) * 256] = total
        if j % 4 == 3:
            part = pl.ds((j - 3) * 256, 1024)
            sent.append(
                pltpu.make_async_copy(image_ref.at[:, part], image_hbm.at[:, part], sems.at[j // 4])
            )
            sent[-1].start()
    for copy in sent:
        copy.wait()


def call(kernel, outs, in_specs, flops, moved, scratch=(), limit=24 * 2**20, out_specs=None):
    return pl.pallas_call(
        kernel,
        out_shape=tuple(jax.ShapeDtypeStruct(s, t) for s, t in outs),
        in_specs=in_specs,
        out_specs=out_specs or tuple(VMEM for _ in outs),
        scratch_shapes=list(scratch),
        compiler_params=pltpu.CompilerParams(vmem_limit_bytes=limit),
        cost_estimate=pl.CostEstimate(flops=flops, bytes_accessed=moved, transcendentals=0),
    )


def exchange(message):
    rows = message.shape[0]
    out = lax.all_to_all(
        message.reshape(rows, 1, LANES), AXES, 0, 0, tiled=True, axis_index_groups=[PLACES]
    )
    return out.reshape(rows, LANES)


def mirror_exchange(grid, edge, alone):
    got = lax.ppermute(edge, AXES, MIRROR_EDGE)
    other = lax.ppermute(grid, AXES, MIRROR)
    return grid, other, edge, got, alone


def per_device(image0, interp, vis_weight, counts, tile_index):
    t = {
        k: tuple(jnp.asarray(a) for a in v) if isinstance(v, tuple) else jnp.asarray(v)
        for k, v in tables().items()
    }
    pack = call(
        pack_kernel,
        [((DEV * MSG, LANES), F32)],
        [HBM] * 6,
        200_000_000,
        5_000_000,
        scratch=[
            pltpu.VMEM((DEV * MSG, LANES), F32),
            pltpu.VMEM((ROWS, N), F32),
            pltpu.VMEM((SLOTS, VCAP, CELLS), F32),
            pltpu.VMEM((VCAP, SLOTS), F32),
            pltpu.VMEM((1, SLOTS), jnp.int32),
            pltpu.VMEM((1, SLOTS), jnp.int32),
            pltpu.VMEM((80, DEV), F32),
            pltpu.VMEM((2, DEV, 2 * DEV), BF16),
            pltpu.SemaphoreType.DMA((21,)),
        ],
        limit=PACK_LIMIT,
        out_specs=(HBM,),
    )
    (message,) = pack(
        image0,
        interp.reshape(SLOTS, VCAP, CELLS),
        vis_weight.reshape(SLOTS, VCAP).T,
        tile_index.reshape(1, SLOTS),
        counts.reshape(1, SLOTS),
        t["start"],
    )
    got = exchange(message)
    (row,) = call(row_kernel, [((DEV, LANES), F32)], [VMEM], 100_000, 300_000)(got)
    other = lax.ppermute(row, AXES, MIRROR)
    a_high, a_low, mask, turned = call(
        unpack_kernel,
        [((SAMPLES, CELLS), BF16), ((SAMPLES, CELLS), BF16), ((16, 256), F32), ((LANES, DEV), F32)],
        [VMEM] * 2,
        100_000_000,
        5_000_000,
    )(got, row)
    first = call(
        first_kernel,
        [((LANES, CELLS), F32), ((32, LANES), F32), ((8, LANES), F32)],
        [VMEM] * 10,
        1_000_000_000,
        3_000_000,
    )
    grid, edge, n0 = first(
        turned, other, a_high, a_low, mask, *t["placed"], t["turn"], *t["eight_fwd"]
    )
    place = lax.axis_index(AXES)
    alone = (place == PLACES[SELF_EDGE[0]]) | (place == PLACES[SELF_EDGE[1]])
    alone = alone.astype(jnp.int32).reshape(1, 1)
    norms = [n0]
    follow = call(
        next_kernel,
        [((LANES, CELLS), F32), ((32, LANES), F32), ((8, LANES), F32)],
        [VMEM] * 4 + [SMEM] + [VMEM] * 5,
        1_000_000_000,
        3_000_000,
    )
    for _ in range(2):
        blocks = mirror_exchange(grid, edge, alone)
        grid, edge, norm = follow(
            *blocks, a_high, a_low, mask, t["flip_tile"], t["flip_cell"]
        )
        norms.append(norm)
    blocks = mirror_exchange(grid, edge, alone)
    send = call(
        send_kernel, [((DEV, LANES), F32)], [VMEM] * 4 + [SMEM] + [VMEM] * 10, 300_000_000, 1_500_000
    )
    (message,) = send(
        *blocks, *norms, t["flip_tile"], t["flip_cell"],
        *t["placed"], t["turn"], *t["eight_inv"],
    )
    got = exchange(message)
    last = call(
        last_kernel,
        [((ROWS, N), F32), ((1, 3), F32)],
        [VMEM] * 5,
        200_000_000,
        1_500_000,
        scratch=[pltpu.VMEM((ROWS, N), F32), pltpu.SemaphoreType.DMA((2,))],
        out_specs=(HBM, VMEM),
    )
    image, found = last(got, t["share"], *t["plain"], t["turn"])
    return image, found.reshape(3)


def solution(mesh):
    in_specs = (
        P(AXES, None),
        P("base", "chan", None, None, None),
        P("base", "chan", None, None),
        P("base", "chan", None),
        P("base", "chan", None),
    )
    return jax.shard_map(
        per_device, mesh=mesh, in_specs=in_specs, out_specs=(P(AXES, None), P()), check_vma=False
    )
```
